32 devices in a mesh: band: 4 (over z), rows: 8 (over y, x, core).
Axes of the slice: x: 2, y: 2, z: 4, core: 2. Of those that a mesh axis runs over, the one named last changes fastest.
Arguments:
- tiles: bfloat16 [8, 4, 4, 512, 512], P('rows', 'band'), may hold values from -0.25 to 0.25
- tile_row: int32 [8, 4, 4], P('rows', 'band'), may hold values from 0 to 3
- tile_col: int32 [8, 4, 4], P('rows', 'band'), may hold values from 0 to 7
- tile_count: int32 [8, 4], P('rows', 'band'), may hold values from 1 to 4, as said below
- damping: float32 [128], replicated, may hold values from 0.5 to 2
- right_side: float32 [16384, 128], P(('rows', 'band')), may hold values from -40 to 40
Outputs:
- basis: float32 [4, 16384, 128], P(None, ('rows', 'band'))
- hessenberg: float32 [4, 3, 128], replicated
The draws below stay inside these ranges and needn't reach their ends.
Inputs may be any that keep to these rules, and one draw needn't show every extreme that they name: `tile_count`: slots at or past the count hold tiles that are not part of the matrix; some row shard and band holds exactly 4 live tiles.
All inputs are finite; a program needn't handle non-finite values.
Results may differ from the reference program's by a relative error of at most 0.007.
Values may be sent and summed in bfloat16 or wider, within the bound.
No kernel may reach another device: no remote copies, remote signals or barrier semaphores. Data moves between devices by JAX's collectives and lax.ppermute only.
A program may use at most 64 MiB of HBM per device.

```python
import math
import jax
import jax.numpy as jnp
from jax import lax

TILE = 512
QUERIES = 128
TILES_DEV = 4
ITERS = 3
NDIM = 16384
N_BAND = 4
N_ROWS = 8


def draw_tile_count(key, part):
    first, second, third = jax.random.split(jax.random.fold_in(key, 17), 3)
    lower = jax.random.randint(first, (N_ROWS, N_BAND), 1, TILES_DEV + 1)
    upper = jax.random.randint(second, (N_ROWS, N_BAND), 1, TILES_DEV + 1)
    counts = jnp.minimum(lower, upper).reshape(-1)
    place = jax.random.randint(third, (), 0, N_ROWS * N_BAND)
    counts = counts.at[place].set(TILES_DEV)
    return counts.reshape(N_ROWS, N_BAND).astype(jnp.int32)


def draw_right_side(key, part):
    first = jax.random.fold_in(jax.random.fold_in(key, 29), 0)
    ramp = 1.0 + 2.0 * jnp.arange(NDIM, dtype=jnp.float32) / (NDIM - 1)
    values = jax.random.normal(first, (NDIM, QUERIES), jnp.float32) * ramp[:, None]
    return jnp.clip(values, -40.0, 40.0).astype(jnp.float32)


def plant(values, rng, least, largest):
    extent = values.shape
    index_at = [jax.random.randint(jax.random.fold_in(rng, axis), (), 0, extent[axis]) for axis in range(len(extent))]
    values = values.at[tuple(index_at)].set(least)
    longest = extent.index(max(extent))
    index_at[longest] = (index_at[longest] + 1) % extent[longest]
    return values.at[tuple(index_at)].set(largest)


def levels(own_key, shape, pieces, smallest, top_value):
    def one(position, blocks):
        draws = jax.random.uniform(jax.random.fold_in(jax.random.fold_in(own_key, 6), position), (blocks,), jnp.float32, smallest / len(pieces), top_value / len(pieces))
        return jnp.repeat(jnp.exp(draws), shape[position] // blocks).reshape((-1,) + (1,) * (len(shape) - position - 1))

    level = one(*pieces[0])
    for cut in pieces[1:]:
        level = level * one(*cut)
    return level


def normal_values(stream_key, shape, width, bound, shards=(), kind=jnp.bfloat16):
    loudness = levels(stream_key, shape, shards, -0.22, 0.18) if shards else 1.0
    drawn = jax.random.normal(stream_key, shape, jnp.float32) * width * loudness
    return jnp.minimum(jnp.maximum(drawn, -bound), bound).astype(kind)


def setup_inputs(seed: int = 0) -> dict:
    streams_of = jax.random.split(jax.random.key(seed), 7)
    return {
        "tiles": normal_values(streams_of[0], (N_ROWS, N_BAND, TILES_DEV, TILE, TILE), TILE ** -0.5, 0.25, ((0, 8), (1, 4))),
        "tile_row": plant(jax.random.randint(streams_of[1], (N_ROWS, N_BAND, TILES_DEV), 0, N_BAND), jax.random.fold_in(streams_of[1], 1), 0, N_BAND - 1).astype(jnp.int32),
        "tile_col": plant(jax.random.randint(streams_of[2], (N_ROWS, N_BAND, TILES_DEV), 0, N_ROWS), jax.random.fold_in(streams_of[2], 1), 0, N_ROWS - 1).astype(jnp.int32),
        "tile_count": draw_tile_count(jax.random.fold_in(streams_of[6], 71), 0),
        "damping": jnp.clip(jnp.exp(jax.random.uniform(streams_of[4], (QUERIES,), jnp.float32, math.log(0.5), math.log(2.0))), 0.5, 2.0),
        "right_side": draw_right_side(jax.random.fold_in(streams_of[6], 71), 0),
    }


EPS = 1e-06

def tile_product(tiles, tile_row, tile_col, tile_count, vector):
    columns = vector.astype(jnp.bfloat16).reshape(N_ROWS, N_BAND, TILE, QUERIES)
    slots = jnp.arange(TILES_DEV).astype(jnp.int32)
    targets = jnp.arange(N_BAND).astype(jnp.int32)

    def row_shard(shard):

        def add_band(running, band):
            band_columns = jnp.take(columns, band, axis=1)
            picked = jnp.take(band_columns, tile_col[shard, band], axis=0).astype(jnp.float32)
            local_tiles = tiles[shard, band].astype(jnp.float32)
            products = jnp.einsum('sij,sjq->siq', local_tiles, picked, precision=lax.Precision.HIGHEST)
            live = slots < tile_count[shard, band]
            onehot = ((tile_row[shard, band][:, None] == targets[None, :]) & live[:, None]).astype(jnp.float32)
            added = jnp.einsum('st,siq->tiq', onehot, products, precision=lax.Precision.HIGHEST)
            return (running + added, None)
        running, unused = lax.scan(add_band, jnp.zeros((N_BAND, TILE, QUERIES), jnp.float32), jnp.arange(N_BAND).astype(jnp.int32))
        return running
    return lax.map(row_shard, jnp.arange(N_ROWS).astype(jnp.int32)).reshape(NDIM, QUERIES)

def reference(tiles, tile_row, tile_col, tile_count, damping, right_side):
    start = lax.optimization_barrier(jnp.sum(right_side * right_side, axis=0))
    vectors = [right_side * lax.rsqrt(start + EPS)[None, :]]
    hessenberg = jnp.zeros((ITERS + 1, ITERS, QUERIES), jnp.float32)
    for step in range(ITERS):
        current = vectors[step]
        image = tile_product(tiles, tile_row, tile_col, tile_count, current) + damping[None, :] * current
        for other in range(step + 1):
            coefficient = lax.optimization_barrier(jnp.sum(vectors[other] * image, axis=0))
            image = image - coefficient[None, :] * vectors[other]
            hessenberg = hessenberg.at[other, step].set(coefficient)
        norm = jnp.sqrt(lax.optimization_barrier(jnp.sum(image * image, axis=0)) + EPS)
        hessenberg = hessenberg.at[step + 1, step].set(norm)
        vectors.append(image / norm[None, :])
    basis = jnp.stack(vectors) * math.sqrt(NDIM)
    return (basis, hessenberg)
```

```python
import functools
import math

import jax
import jax.numpy as jnp
from jax import lax
from jax.experimental import pallas as pl
from jax.experimental.pallas import tpu as pltpu
from jax.sharding import PartitionSpec as P

ITERS = 3
EPS = 1e-06
EXTRA = 16
F32 = jnp.float32
BF16 = jnp.bfloat16


def partners(size, step):
    if size & (size - 1) == 0:
        return [(i, i ^ step) for i in range(size)]
    return [(i, (i + step) % size) for i in range(size)]


def exchange_of(target, own, size):
    if size & (size - 1) == 0:
        return target ^ own
    return (target - own + size) % size


def pieces(value):
    high = value.astype(BF16).astype(F32)
    rest = value - high
    middle = rest.astype(BF16).astype(F32)
    return [high, middle, rest - middle]


def pack_rows(rows, count):
    place = lax.broadcasted_iota(jnp.int32, (count, rows[0].shape[1]), 0)
    packed = jnp.zeros(place.shape, F32)
    for index, row in enumerate(rows):
        packed = jnp.where(place == index, row, packed)
    return packed


def row_of(packed, index):
    return packed[index : index + 1, :]


def sum_of(packed, index):
    return row_of(packed, index) + row_of(packed, index + 1) + row_of(packed, index + 2)


def ratio(top, bottom):
    safe = jnp.where(bottom > 0, bottom, 1.0)
    return jnp.where(bottom > 0, top / safe, 0.0).astype(BF16).astype(F32)


def over_rows(value):
    return jnp.sum(value, axis=0, keepdims=True)


def round_kernel(right_side, message):
    message[...] = right_side[...].astype(BF16)


def product_kernel(step, shards, bands, slots, width, *refs):
    refs = list(refs)
    take = lambda n: [refs.pop(0) for _ in range(n)]
    count_ref, row_ref, col_ref, tiles = take(4)
    blocks = take(shards)
    older = take(step)
    side, coefs = take(2) if step == 2 else (None, None)
    outs = take(bands)
    stored = take(1)[0] if step < ITERS - 1 else None
    side_out = take(1)[0] if step == 1 else None
    column, extras, total = take(3)
    shard = lax.axis_index("rows")
    band = lax.axis_index("band")
    total[...] = jnp.zeros(total.shape, F32)
    rows = []
    wholes = []
    if step:
        for k in range(shards):
            extras[k] = blocks[k][width:, :].astype(F32)
        added = extras[0]
        for k in range(1, shards):
            added = added + extras[k]
        sums = [sum_of(added, step + 3 * i) for i in range(2 if step == 1 else 4)]
        if step == 1:
            wholes = [ratio(sums[0], sums[1])]
        else:
            inner_0, inner_1, norm_1, cross = sums
            whole_1 = ratio(inner_1, norm_1)
            wholes = [ratio(inner_0 - whole_1 * cross, side[slots : slots + 1, :]), whole_1]
        rows = wholes + [piece for value in sums for piece in pieces(value)]
    if side_out is not None:
        side_out[...] = jnp.zeros(side_out.shape, F32)
        side_out[slots : slots + 1, :] = sums[1]
    for slot in range(slots):

        @pl.when(slot < count_ref[0, 0])
        def _(slot=slot):
            source = exchange_of(col_ref[0, 0, slot], shard, shards)
            target = exchange_of(row_ref[0, 0, slot], band, bands)
            for k in range(shards):

                @pl.when(source == k)
                def _(k=k):
                    column[...] = blocks[k][:width, :]

            product = jnp.dot(tiles[0, 0, slot], column[...], preferred_element_type=F32)
            if stored is not None:
                stored[slot] = product
            if step:
                extra = extras[source]
                if step == 1:
                    own = row_of(extra, 0)
                    side_out[slot : slot + 1, :] = own
                    product = product + (own - wholes[0]) * older[0][slot]
                else:
                    first = row_of(extra, 0) - wholes[0]
                    second = row_of(extra, 1) - wholes[1]
                    first = first + second * (side[slot : slot + 1, :] - coefs[0:1, :])
                    product = product + second * older[1][slot] + first * older[0][slot]
            total[target] += product

    outs[0][:width, :] = total[0]
    for k in range(1, bands):
        outs[k][:width, :] = total[k].astype(BF16)
    if step:
        packed = pack_rows(rows, EXTRA)
        outs[0][width:, :] = packed
        for k in range(1, bands):
            outs[k][width:, :] = packed.astype(BF16)


def message_of(message, value, coefs, sums):
    width = value.shape[0]
    message[:width, :] = value.astype(BF16)
    rows = coefs + [piece for entry in sums for piece in pieces(entry)]
    message[width:, :] = pack_rows(rows, EXTRA).astype(BF16)


def first_kernel(bands, damping, r_0, *refs):
    parts = refs[:bands]
    image_out, message = refs[bands:]
    r = r_0[...]
    image = damping[...] * r
    for part in parts:
        image = image + part[...].astype(F32)
    image_out[...] = image
    inner = over_rows(r * image)
    norm = over_rows(r * r)
    own = ratio(inner, norm)
    message_of(message, image - own * r, [own], [inner, norm])


def global_sums(parts, width, step, count):
    packed = parts[0][width:, :].astype(F32)
    for part in parts[1:]:
        packed = packed + part[width:, :].astype(F32)
    return [sum_of(packed, step + 3 * i) for i in range(count)]


def second_kernel(bands, damping, r_0, image_0, *refs):
    first = refs[:bands]
    parts = refs[bands : 2 * bands]
    r_1_out, image_out, message, coefs = refs[2 * bands :]
    width = r_0.shape[0]
    inner, norm = global_sums(parts, width, 1, 2)
    scale_0 = norm + EPS
    taken = inner / scale_0
    r0 = r_0[...]
    r1 = image_0[...] - taken * r0
    r_1_out[...] = r1
    image = damping[...] * r1
    for old, part in zip(first, parts):
        back = part[width : width + 1, :].astype(F32) - taken
        image = image + part[:width, :].astype(F32) + back * old[...].astype(F32)
    image_out[...] = image
    inner_0 = over_rows(r0 * image)
    inner_1 = over_rows(r1 * image)
    norm_1 = over_rows(r1 * r1)
    cross = over_rows(r0 * r1)
    own_1 = ratio(inner_1, norm_1)
    rest = image - own_1 * r1
    own_0 = ratio(over_rows(r0 * rest), over_rows(r0 * r0))
    message_of(message, rest - own_0 * r0, [own_0, own_1], [inner_0, inner_1, norm_1, cross])
    coefs[...] = pack_rows([taken, scale_0], 8)


def third_kernel(bands, damping, r_0, r_1, image_1, coefs, *refs):
    first = refs[:bands]
    second = refs[bands : 2 * bands]
    parts = refs[2 * bands : 3 * bands]
    r_2_out, image_out, sums_out, coefs_out = refs[3 * bands :]
    width = r_0.shape[0]
    inner_0, inner_1, norm_1, cross = global_sums(parts, width, 2, 4)
    taken_00 = coefs[0:1, :]
    scale_0 = coefs[1:2, :]
    scale_1 = norm_1 + EPS * scale_0
    taken_0 = inner_0 / scale_0
    taken_1 = (inner_1 - taken_0 * cross) / scale_1
    r0 = r_0[...]
    r1 = r_1[...]
    r2 = image_1[...] - taken_0 * r0 - taken_1 * r1
    r_2_out[...] = r2
    image = damping[...] * r2
    for old_0, old_1, part in zip(first, second, parts):
        back_0 = part[width : width + 1, :].astype(F32) - taken_0
        back_1 = part[width + 1 : width + 2, :].astype(F32) - taken_1
        back_0 = back_0 + back_1 * (old_1[width : width + 1, :].astype(F32) - taken_00)
        image = image + part[:width, :].astype(F32)
        image = image + back_1 * old_1[:width, :].astype(F32) + back_0 * old_0[...].astype(F32)
    image_out[...] = image
    pairs = ((r0, image), (r1, image), (r2, image), (r2, r2), (image, image), (r0, r2), (r1, r2))
    sums_out[...] = pack_rows([over_rows(a * b) for a, b in pairs], 8)
    coefs_out[...] = pack_rows([taken_00, taken_0, taken_1, scale_0, scale_1, cross, norm_1], 8)


def last_kernel(rescale, coefs, sums, r_0, r_1, r_2, image_2, basis, hessenberg):
    total = sums[0]
    for k in range(1, sums.shape[0]):
        total = total + sums[k]
    inner_0, inner_1, inner_2, norm_2, square, cross_02, cross_12 = [row_of(total, i) for i in range(7)]
    taken_00, taken_01, taken_11, scale_0, scale_1, cross_01, norm_1 = [coefs[i : i + 1, :] for i in range(7)]
    norm_0 = scale_0 - EPS
    scale_2 = norm_2 + EPS * scale_1
    taken_0 = inner_0 / scale_0
    taken_1 = (inner_1 - taken_0 * cross_01) / scale_1
    taken_2 = (inner_2 - taken_0 * cross_02 - taken_1 * cross_12) / scale_2
    square = square - taken_0 * (2.0 * inner_0 - taken_0 * norm_0)
    square = square - taken_1 * (2.0 * (inner_1 - taken_0 * cross_01) - taken_1 * norm_1)
    square = square - taken_2 * (2.0 * (inner_2 - taken_0 * cross_02 - taken_1 * cross_12) - taken_2 * norm_2)
    scale_3 = jnp.maximum(square, 0.0) + EPS * scale_2
    inverse = [lax.rsqrt(scale) for scale in (scale_0, scale_1, scale_2, scale_3)]
    root = [scale * inv for scale, inv in zip((scale_0, scale_1, scale_2, scale_3), inverse)]
    image = image_2[...] - taken_0 * r_0[...] - taken_1 * r_1[...] - taken_2 * r_2[...]
    basis[0] = r_0[...] * (inverse[0] * rescale)
    basis[1] = r_1[...] * (inverse[1] * rescale)
    basis[2] = r_2[...] * (inverse[2] * rescale)
    basis[3] = image * (inverse[3] * rescale)
    hessenberg[...] = jnp.zeros(hessenberg.shape, F32)
    for step, column in enumerate(((taken_00,), (taken_01, taken_11), (taken_0, taken_1, taken_2))):
        for i, taken in enumerate(column):
            hessenberg[i, step : step + 1, :] = taken * root[i] * inverse[step]
        hessenberg[step + 1, step : step + 1, :] = root[step + 1] * inverse[step]


def call(kernel, outs, *operands, scalars=0, scratch=()):
    vmem = pl.BlockSpec(memory_space=pltpu.VMEM)
    smem = pl.BlockSpec(memory_space=pltpu.SMEM)
    return pl.pallas_call(
        kernel,
        out_shape=[jax.ShapeDtypeStruct(shape, dtype) for shape, dtype in outs],
        in_specs=[smem] * scalars + [vmem] * (len(operands) - scalars),
        out_specs=[vmem] * len(outs),
        scratch_shapes=list(scratch),
    )(*operands)


def gather(message, shards):
    blocks = [None] * shards
    blocks[0] = message
    for k in range(2, shards, 2):
        blocks[k] = lax.ppermute(message, "rows", partners(shards, k))
    for k in range(0, shards, 2):
        blocks[k + 1] = lax.ppermute(blocks[k], "rows", partners(shards, 1))
    return blocks


def on_device(tiles, tile_row, tile_col, tile_count, damping, right_side):
    bands = lax.axis_size("band")
    shards = lax.axis_size("rows")
    slots = tiles.shape[2]
    width = right_side.shape[0]
    queries = right_side.shape[1]
    rescale = math.sqrt(width * bands * shards)
    damping = damping.reshape(1, queries)
    block = ((width, queries), F32)
    long_message = ((width + EXTRA, queries), BF16)
    small = ((8, queries), F32)

    def multiply(step, message, *older):
        blocks = gather(message, shards)
        extra = EXTRA if step else 0
        outs = [((width + extra, queries), F32)] + [((width + extra, queries), BF16)] * (bands - 1)
        if step < ITERS - 1:
            outs.append(((slots, width, queries), F32))
        if step == 1:
            outs.append(((slots + 8 - slots % 8, queries), F32))
        results = call(
            functools.partial(product_kernel, step, shards, bands, slots, width),
            outs,
            tile_count,
            tile_row,
            tile_col,
            tiles,
            *blocks,
            *older,
            scalars=3,
            scratch=(
                pltpu.VMEM((width, queries), BF16),
                pltpu.VMEM((shards, EXTRA, queries), F32),
                pltpu.VMEM((bands, width, queries), F32),
            ),
        )
        parts = [results[0]] + [lax.ppermute(results[k], "band", partners(bands, k)) for k in range(1, bands)]
        return parts, list(results[bands:])

    (message,) = call(round_kernel, [((width, queries), BF16)], right_side)
    parts_0, (stored_0,) = multiply(0, message)
    image_0, message = call(functools.partial(first_kernel, bands), [block, long_message], damping, right_side, *parts_0)
    parts_1, (stored_1, side) = multiply(1, message, stored_0)
    r_1, image_1, message, coefs = call(
        functools.partial(second_kernel, bands), [block, block, long_message, small], damping, right_side, image_0, *parts_0, *parts_1
    )
    parts_2, _ = multiply(2, message, stored_0, stored_1, side, coefs)
    r_2, image_2, sums, coefs = call(
        functools.partial(third_kernel, bands),
        [block, block, small, small],
        damping,
        right_side,
        r_1,
        image_1,
        coefs,
        *parts_0,
        *parts_1,
        *parts_2,
    )
    everyone = jnp.broadcast_to(sums[None], (bands * shards, *sums.shape))
    everyone = lax.all_to_all(everyone, ("rows", "band"), 0, 0, tiled=True)
    return call(
        functools.partial(last_kernel, rescale),
        [((ITERS + 1, width, queries), F32), ((ITERS + 1, ITERS, queries), F32)],
        coefs,
        everyone,
        right_side,
        r_1,
        r_2,
        image_2,
    )


def solution(mesh):
    return jax.shard_map(
        lambda *args: tuple(on_device(*args)),
        mesh=mesh,
        in_specs=(
            P("rows", "band", None, None, None),
            P("rows", "band", None),
            P("rows", "band", None),
            P("rows", "band"),
            P(),
            P(("rows", "band"), None),
        ),
        out_specs=(P(None, ("rows", "band"), None), P()),
        check_vma=False,
    )
```

```python
import functools
import math

import jax
import jax.numpy as jnp
from jax import lax
from jax.experimental import pallas as pl
from jax.experimental.pallas import tpu as pltpu
from jax.sharding import PartitionSpec as P

ITERS = 3
EPS = 1e-06
EXTRA = 16
VMEM_LIMIT = 16 << 20
F32 = jnp.float32
BF16 = jnp.bfloat16


def partners(size, step):
    return [(i, i ^ step) for i in range(size)]


def pieces(value):
    high = value.astype(BF16).astype(F32)
    rest = value - high
    middle = rest.astype(BF16).astype(F32)
    return [high, middle, rest - middle]


def pack_rows(rows, count):
    place = lax.broadcasted_iota(jnp.int32, (count, rows[0].shape[1]), 0)
    packed = jnp.zeros(place.shape, F32)
    for index, row in enumerate(rows):
        packed = jnp.where(place == index, row, packed)
    return packed


def row_of(packed, index):
    return packed[index : index + 1, :]


def sum_of(packed, index):
    return row_of(packed, index) + row_of(packed, index + 1) + row_of(packed, index + 2)


def ratio(top, bottom):
    safe = jnp.where(bottom > 0, bottom, 1.0)
    return jnp.where(bottom > 0, top / safe, 0.0).astype(BF16).astype(F32)


def over_rows(value):
    return jnp.sum(value, axis=0, keepdims=True)


def open_kernel(tiles, right_side, row, col, count, staged, r_0, message, plan, rows, cols, sems):
    slots = row.shape[2]
    moves = [
        pltpu.make_async_copy(source, target, sems.at[i])
        for i, (source, target) in enumerate(
            ((right_side, r_0), (row, rows), (col, cols), (tiles.at[0, 0], staged))
        )
    ]
    for move in moves:
        move.start()
    moves[0].wait()
    message[...] = r_0[...].astype(BF16)
    for move in moves[1:3]:
        move.wait()
    plan[0, 0] = count[0, 0]
    shard = lax.axis_index("rows")
    band = lax.axis_index("band")
    for slot in range(slots):
        plan[0, 1 + slot] = cols[0, 0, slot] ^ shard
        plan[0, 1 + slots + slot] = rows[0, 0, slot] ^ band
    moves[3].wait()


def product_kernel(step, shards, bands, slots, width, *refs):
    refs = list(refs)
    take = lambda n: [refs.pop(0) for _ in range(n)]
    plan, tiles = take(2)
    blocks = take(shards)
    older = take(step)
    side, coefs = take(2) if step == 2 else (None, None)
    outs = take(bands)
    stored = take(1)[0] if step < ITERS - 1 else None
    side_out = take(1)[0] if step == 1 else None
    column, extras, total = take(3)
    total[...] = jnp.zeros(total.shape, F32)
    rows = []
    wholes = []
    if step:
        for k in range(shards):
            extras[k] = blocks[k][width:, :].astype(F32)
        added = extras[0]
        for k in range(1, shards):
            added = added + extras[k]
        sums = [sum_of(added, step + 3 * i) for i in range(2 if step == 1 else 4)]
        if step == 1:
            wholes = [ratio(sums[0], sums[1])]
        else:
            inner_0, inner_1, norm_1, cross = sums
            whole_1 = ratio(inner_1, norm_1)
            wholes = [ratio(inner_0 - whole_1 * cross, side[slots : slots + 1, :]), whole_1]
        rows = wholes + [piece for value in sums for piece in pieces(value)]
    if side_out is not None:
        side_out[...] = jnp.zeros(side_out.shape, F32)
        side_out[slots : slots + 1, :] = sums[1]
    for slot in range(slots):

        @pl.when(slot < plan[0, 0])
        def _(slot=slot):
            source = plan[0, 1 + slot]
            target = plan[0, 1 + slots + slot]
            for k in range(shards):

                @pl.when(source == k)
                def _(k=k):
                    column[...] = blocks[k][:width, :]

            product = jnp.dot(tiles[slot], column[...], preferred_element_type=F32)
            if stored is not None:
                stored[slot] = product
            if step:
                extra = extras[source]
                if step == 1:
                    own = row_of(extra, 0)
                    side_out[slot : slot + 1, :] = own
                    product = product + (own - wholes[0]) * older[0][slot]
                else:
                    first = row_of(extra, 0) - wholes[0]
                    second = row_of(extra, 1) - wholes[1]
                    first = first + second * (side[slot : slot + 1, :] - coefs[0:1, :])
                    product = product + second * older[1][slot] + first * older[0][slot]
            total[target] += product

    outs[0][:width, :] = total[0]
    for k in range(1, bands):
        outs[k][:width, :] = total[k].astype(BF16)
    if step:
        packed = pack_rows(rows, EXTRA)
        outs[0][width:, :] = packed
        for k in range(1, bands):
            outs[k][width:, :] = packed.astype(BF16)


def message_of(message, value, coefs, sums):
    width = value.shape[0]
    message[:width, :] = value.astype(BF16)
    rows = coefs + [piece for entry in sums for piece in pieces(entry)]
    message[width:, :] = pack_rows(rows, EXTRA).astype(BF16)


def first_kernel(bands, damping, r_0, *refs):
    parts = refs[:bands]
    image_out, message = refs[bands:]
    r = r_0[...]
    image = damping[...] * r
    for part in parts:
        image = image + part[...].astype(F32)
    image_out[...] = image
    inner = over_rows(r * image)
    norm = over_rows(r * r)
    own = ratio(inner, norm)
    message_of(message, image - own * r, [own], [inner, norm])


def global_sums(parts, width, step, count):
    packed = parts[0][width:, :].astype(F32)
    for part in parts[1:]:
        packed = packed + part[width:, :].astype(F32)
    return [sum_of(packed, step + 3 * i) for i in range(count)]


def second_kernel(bands, damping, r_0, image_0, *refs):
    first = refs[:bands]
    parts = refs[bands : 2 * bands]
    r_1_out, image_out, message, coefs = refs[2 * bands :]
    width = r_0.shape[0]
    inner, norm = global_sums(parts, width, 1, 2)
    scale_0 = norm + EPS
    taken = inner / scale_0
    r0 = r_0[...]
    r1 = image_0[...] - taken * r0
    r_1_out[...] = r1
    image = damping[...] * r1
    for old, part in zip(first, parts):
        back = part[width : width + 1, :].astype(F32) - taken
        image = image + part[:width, :].astype(F32) + back * old[...].astype(F32)
    image_out[...] = image
    inner_0 = over_rows(r0 * image)
    inner_1 = over_rows(r1 * image)
    norm_1 = over_rows(r1 * r1)
    cross = over_rows(r0 * r1)
    own_1 = ratio(inner_1, norm_1)
    rest = image - own_1 * r1
    own_0 = ratio(over_rows(r0 * rest), over_rows(r0 * r0))
    message_of(message, rest - own_0 * r0, [own_0, own_1], [inner_0, inner_1, norm_1, cross])
    coefs[...] = pack_rows([taken, scale_0], 8)


def third_kernel(bands, damping, r_0, r_1, image_1, coefs, *refs):
    first = refs[:bands]
    second = refs[bands : 2 * bands]
    parts = refs[2 * bands : 3 * bands]
    r_2_out, image_out, sums_out, coefs_out = refs[3 * bands :]
    width = r_0.shape[0]
    inner_0, inner_1, norm_1, cross = global_sums(parts, width, 2, 4)
    taken_00 = coefs[0:1, :]
    scale_0 = coefs[1:2, :]
    scale_1 = norm_1 + EPS * scale_0
    taken_0 = inner_0 / scale_0
    taken_1 = (inner_1 - taken_0 * cross) / scale_1
    r0 = r_0[...]
    r1 = r_1[...]
    r2 = image_1[...] - taken_0 * r0 - taken_1 * r1
    r_2_out[...] = r2
    image = damping[...] * r2
    for old_0, old_1, part in zip(first, second, parts):
        back_0 = part[width : width + 1, :].astype(F32) - taken_0
        back_1 = part[width + 1 : width + 2, :].astype(F32) - taken_1
        back_0 = back_0 + back_1 * (old_1[width : width + 1, :].astype(F32) - taken_00)
        image = image + part[:width, :].astype(F32)
        image = image + back_1 * old_1[:width, :].astype(F32) + back_0 * old_0[...].astype(F32)
    image_out[...] = image
    pairs = ((r0, image), (r1, image), (r2, image), (r2, r2), (image, image), (r0, r2), (r1, r2))
    sums_out[...] = pack_rows([over_rows(a * b) for a, b in pairs], 8)
    coefs_out[...] = pack_rows([taken_00, taken_0, taken_1, scale_0, scale_1, cross, norm_1], 8)


def last_kernel(rescale, coefs, sums, r_0, r_1, r_2, image_2, basis_out, hessenberg_out, basis, hessenberg, sems):
    total = sums[0]
    for k in range(1, sums.shape[0]):
        total = total + sums[k]
    inner_0, inner_1, inner_2, norm_2, square, cross_02, cross_12 = [row_of(total, i) for i in range(7)]
    taken_00, taken_01, taken_11, scale_0, scale_1, cross_01, norm_1 = [coefs[i : i + 1, :] for i in range(7)]
    norm_0 = scale_0 - EPS
    scale_2 = norm_2 + EPS * scale_1
    taken_0 = inner_0 / scale_0
    taken_1 = (inner_1 - taken_0 * cross_01) / scale_1
    taken_2 = (inner_2 - taken_0 * cross_02 - taken_1 * cross_12) / scale_2
    square = square - taken_0 * (2.0 * inner_0 - taken_0 * norm_0)
    square = square - taken_1 * (2.0 * (inner_1 - taken_0 * cross_01) - taken_1 * norm_1)
    square = square - taken_2 * (2.0 * (inner_2 - taken_0 * cross_02 - taken_1 * cross_12) - taken_2 * norm_2)
    scale_3 = jnp.maximum(square, 0.0) + EPS * scale_2
    inverse = [lax.rsqrt(scale) for scale in (scale_0, scale_1, scale_2, scale_3)]
    root = [scale * inv for scale, inv in zip((scale_0, scale_1, scale_2, scale_3), inverse)]
    moves = [pltpu.make_async_copy(basis.at[i], basis_out.at[i], sems.at[i]) for i in range(ITERS + 1)]
    moves.append(pltpu.make_async_copy(hessenberg, hessenberg_out, sems.at[ITERS + 1]))
    for i, vector in enumerate((r_0, r_1, r_2)):
        basis[i] = vector[...] * (inverse[i] * rescale)
        moves[i].start()
    image = image_2[...] - taken_0 * r_0[...] - taken_1 * r_1[...] - taken_2 * r_2[...]
    basis[3] = image * (inverse[3] * rescale)
    moves[3].start()
    hessenberg[...] = jnp.zeros(hessenberg.shape, F32)
    for step, column in enumerate(((taken_00,), (taken_01, taken_11), (taken_0, taken_1, taken_2))):
        for i, taken in enumerate(column):
            hessenberg[step, i : i + 1, :] = taken * root[i] * inverse[step]
        hessenberg[step, step + 1 : step + 2, :] = root[step + 1] * inverse[step]
    moves[4].start()
    for move in moves:
        move.wait()


def call(kernel, outs, *operands, scalars=0, scratch=()):
    vmem = pl.BlockSpec(memory_space=pltpu.VMEM)
    smem = pl.BlockSpec(memory_space=pltpu.SMEM)
    spaces = [pltpu.SMEM] * scalars + [pltpu.VMEM] * (len(operands) - scalars)
    operands = [pltpu.with_memory_space_constraint(x, space) for x, space in zip(operands, spaces)]
    return pl.pallas_call(
        kernel,
        out_shape=[pltpu.VMEM(shape, dtype) for shape, dtype in outs],
        in_specs=[smem] * scalars + [vmem] * (len(operands) - scalars),
        out_specs=[vmem] * len(outs),
        scratch_shapes=list(scratch),
        compiler_params=pltpu.CompilerParams(vmem_limit_bytes=VMEM_LIMIT),
    )(*operands)


def gather(message, shards):
    blocks = [None] * shards
    blocks[0] = message
    for k in range(2, shards, 2):
        blocks[k] = lax.ppermute(message, "rows", partners(shards, k))
    for k in range(0, shards, 2):
        blocks[k + 1] = lax.ppermute(blocks[k], "rows", partners(shards, 1))
    return blocks


def on_device(tiles, tile_row, tile_col, tile_count, damping, right_side):
    bands = lax.axis_size("band")
    shards = lax.axis_size("rows")
    slots = tiles.shape[2]
    width = right_side.shape[0]
    queries = right_side.shape[1]
    rescale = math.sqrt(width * bands * shards)
    damping = damping.reshape(1, queries)
    block = ((width, queries), F32)
    long_message = ((width + EXTRA, queries), BF16)
    small = ((8, queries), F32)

    def multiply(step, message, *older):
        blocks = gather(message, shards)
        extra = EXTRA if step else 0
        outs = [((width + extra, queries), F32)] + [((width + extra, queries), BF16)] * (bands - 1)
        if step < ITERS - 1:
            outs.append(((slots, width, queries), F32))
        if step == 1:
            outs.append(((slots + 8 - slots % 8, queries), F32))
        results = call(
            functools.partial(product_kernel, step, shards, bands, slots, width),
            outs,
            plan,
            staged,
            *blocks,
            *older,
            scalars=1,
            scratch=(
                pltpu.VMEM((width, queries), BF16),
                pltpu.VMEM((shards, EXTRA, queries), F32),
                pltpu.VMEM((bands, width, queries), F32),
            ),
        )
        parts = [results[0]] + [lax.ppermute(results[k], "band", partners(bands, k)) for k in range(1, bands)]
        return parts, list(results[bands:])

    smem = pl.BlockSpec(memory_space=pltpu.SMEM)
    vmem = pl.BlockSpec(memory_space=pltpu.VMEM)
    staged, right_side, message, plan = pl.pallas_call(
        open_kernel,
        out_shape=[
            pltpu.VMEM(tiles.shape[2:], BF16),
            pltpu.VMEM((width, queries), F32),
            pltpu.VMEM((width, queries), BF16),
            pltpu.SMEM((1, 1 + 2 * slots), jnp.int32),
        ],
        in_specs=[pl.BlockSpec(memory_space=pltpu.HBM)] * 4 + [smem],
        out_specs=[vmem] * 3 + [smem],
        scratch_shapes=[
            pltpu.SMEM(tile_row.shape, jnp.int32),
            pltpu.SMEM(tile_col.shape, jnp.int32),
            pltpu.SemaphoreType.DMA((4,)),
        ],
        compiler_params=pltpu.CompilerParams(vmem_limit_bytes=VMEM_LIMIT),
    )(*[pltpu.with_memory_space_constraint(x, pltpu.HBM) for x in (tiles, right_side, tile_row, tile_col)], tile_count)
    parts_0, (stored_0,) = multiply(0, message)
    image_0, message = call(functools.partial(first_kernel, bands), [block, long_message], damping, right_side, *parts_0)
    parts_1, (stored_1, side) = multiply(1, message, stored_0)
    r_1, image_1, message, coefs = call(
        functools.partial(second_kernel, bands), [block, block, long_message, small], damping, right_side, image_0, *parts_0, *parts_1
    )
    parts_2, _ = multiply(2, message, stored_0, stored_1, side, coefs)
    r_2, image_2, sums, coefs = call(
        functools.partial(third_kernel, bands),
        [block, block, small, small],
        damping,
        right_side,
        r_1,
        image_1,
        coefs,
        *parts_0,
        *parts_1,
        *parts_2,
    )
    everyone = jnp.broadcast_to(sums[None], (bands * shards, *sums.shape))
    everyone = lax.all_to_all(everyone, ("rows", "band"), 0, 0, tiled=True)
    shapes = ((ITERS + 1, width, queries), (ITERS, ITERS + 1, queries))
    basis, hessenberg = pl.pallas_call(
        functools.partial(last_kernel, rescale),
        out_shape=[jax.ShapeDtypeStruct(shape, F32) for shape in shapes],
        in_specs=[vmem] * 6,
        out_specs=[pl.BlockSpec(memory_space=pltpu.HBM)] * 2,
        scratch_shapes=[pltpu.VMEM(shape, F32) for shape in shapes] + [pltpu.SemaphoreType.DMA((ITERS + 2,))],
        compiler_params=pltpu.CompilerParams(vmem_limit_bytes=VMEM_LIMIT),
    )(*[pltpu.with_memory_space_constraint(x, pltpu.VMEM) for x in (coefs, everyone, right_side, r_1, r_2, image_2)])
    return basis, jnp.swapaxes(hessenberg, 0, 1)


def solution(mesh):
    return jax.shard_map(
        lambda *args: tuple(on_device(*args)),
        mesh=mesh,
        in_specs=(
            P("rows", "band", None, None, None),
            P("rows", "band", None),
            P("rows", "band", None),
            P("rows", "band"),
            P(),
            P(("rows", "band"), None),
        ),
        out_specs=(P(None, ("rows", "band"), None), P()),
        check_vma=False,
    )
```

```python
import functools
import math

import jax
import jax.numpy as jnp
from jax import lax
from jax.experimental import pallas as pl
from jax.experimental.pallas import tpu as pltpu
from jax.sharding import PartitionSpec as P

ITERS = 3
EPS = 1e-06
EXTRA = 16
VMEM_LIMIT = 16 << 20
F32 = jnp.float32
BF16 = jnp.bfloat16


def partners(size, step):
    return [(i, i ^ step) for i in range(size)]


def pieces(value):
    high = value.astype(BF16).astype(F32)
    rest = value - high
    middle = rest.astype(BF16).astype(F32)
    return [high, middle, rest - middle]


def pack_rows(rows, count):
    place = lax.broadcasted_iota(jnp.int32, (count, rows[0].shape[1]), 0)
    packed = jnp.zeros(place.shape, F32)
    for index, row in enumerate(rows):
        packed = jnp.where(place == index, row, packed)
    return packed


def row_of(packed, index):
    return packed[index : index + 1, :]


def sum_of(packed, index):
    return row_of(packed, index) + row_of(packed, index + 1) + row_of(packed, index + 2)


def ratio(top, bottom):
    safe = jnp.where(bottom > 0, bottom, 1.0)
    return jnp.where(bottom > 0, top / safe, 0.0).astype(BF16).astype(F32)


def over_rows(value):
    return jnp.sum(value, axis=0, keepdims=True)


def open_kernel(right_side, r_0, message, sem):
    move = pltpu.make_async_copy(right_side, r_0, sem)
    move.start()
    move.wait()
    message[...] = r_0[...].astype(BF16)


def stage_kernel(tiles, row, col, count, after, staged, plan, rows, cols, sems):
    del after
    slots = row.shape[2]
    pairs = ((row, rows), (col, cols), (tiles.at[0, 0], staged))
    moves = [pltpu.make_async_copy(source, target, sems.at[i]) for i, (source, target) in enumerate(pairs)]
    for move in moves:
        move.start()
    for move in moves[:2]:
        move.wait()
    plan[0, 0] = count[0, 0]
    shard = lax.axis_index("rows")
    band = lax.axis_index("band")
    for slot in range(slots):
        plan[0, 1 + slot] = cols[0, 0, slot] ^ shard
        plan[0, 1 + slots + slot] = rows[0, 0, slot] ^ band
    moves[2].wait()


def product_kernel(step, shards, bands, slots, width, *refs):
    refs = list(refs)
    take = lambda n: [refs.pop(0) for _ in range(n)]
    plan, tiles = take(2)
    blocks = take(shards)
    older = take(step)
    side, coefs = take(2) if step == 2 else (None, None)
    outs = take(bands)
    stored = take(1)[0] if step < ITERS - 1 else None
    side_out = take(1)[0] if step == 1 else None
    column, extras, total = take(3)
    total[...] = jnp.zeros(total.shape, F32)
    rows = []
    wholes = []
    if step:
        for k in range(shards):
            extras[k] = blocks[k][width:, :].astype(F32)
        added = extras[0]
        for k in range(1, shards):
            added = added + extras[k]
        sums = [sum_of(added, step + 3 * i) for i in range(2 if step == 1 else 4)]
        if step == 1:
            wholes = [ratio(sums[0], sums[1])]
        else:
            inner_0, inner_1, norm_1, cross = sums
            whole_1 = ratio(inner_1, norm_1)
            wholes = [ratio(inner_0 - whole_1 * cross, side[slots : slots + 1, :]), whole_1]
        rows = wholes + [piece for value in sums for piece in pieces(value)]
    if side_out is not None:
        side_out[...] = jnp.zeros(side_out.shape, F32)
        side_out[slots : slots + 1, :] = sums[1]
    for slot in range(slots):

        @pl.when(slot < plan[0, 0])
        def _(slot=slot):
            source = plan[0, 1 + slot]
            target = plan[0, 1 + slots + slot]
            for k in range(shards):

                @pl.when(source == k)
                def _(k=k):
                    column[...] = blocks[k][:width, :]

            product = jnp.dot(tiles[slot], column[...], preferred_element_type=F32)
            if stored is not None:
                stored[slot] = product
            if step:
                extra = extras[source]
                if step == 1:
                    own = row_of(extra, 0)
                    side_out[slot : slot + 1, :] = own
                    product = product + (own - wholes[0]) * older[0][slot]
                else:
                    first = row_of(extra, 0) - wholes[0]
                    second = row_of(extra, 1) - wholes[1]
                    first = first + second * (side[slot : slot + 1, :] - coefs[0:1, :])
                    product = product + second * older[1][slot] + first * older[0][slot]
            total[target] += product

    outs[0][:width, :] = total[0]
    for k in range(1, bands):
        outs[k][:width, :] = total[k].astype(BF16)
    if step:
        packed = pack_rows(rows, EXTRA)
        outs[0][width:, :] = packed
        for k in range(1, bands):
            outs[k][width:, :] = packed.astype(BF16)


def message_of(message, value, coefs, sums):
    width = value.shape[0]
    message[:width, :] = value.astype(BF16)
    rows = coefs + [piece for entry in sums for piece in pieces(entry)]
    message[width:, :] = pack_rows(rows, EXTRA).astype(BF16)


def first_kernel(bands, damping, r_0, *refs):
    parts = refs[:bands]
    image_out, message = refs[bands:]
    r = r_0[...]
    image = damping[...] * r
    for part in parts:
        image = image + part[...].astype(F32)
    image_out[...] = image
    inner = over_rows(r * image)
    norm = over_rows(r * r)
    own = ratio(inner, norm)
    message_of(message, image - own * r, [own], [inner, norm])


def global_sums(parts, width, step, count):
    packed = parts[0][width:, :].astype(F32)
    for part in parts[1:]:
        packed = packed + part[width:, :].astype(F32)
    return [sum_of(packed, step + 3 * i) for i in range(count)]


def second_kernel(bands, damping, r_0, image_0, *refs):
    first = refs[:bands]
    parts = refs[bands : 2 * bands]
    r_1_out, image_out, message, coefs = refs[2 * bands :]
    width = r_0.shape[0]
    inner, norm = global_sums(parts, width, 1, 2)
    scale_0 = norm + EPS
    taken = inner / scale_0
    r0 = r_0[...]
    r1 = image_0[...] - taken * r0
    r_1_out[...] = r1
    image = damping[...] * r1
    for old, part in zip(first, parts):
        back = part[width : width + 1, :].astype(F32) - taken
        image = image + part[:width, :].astype(F32) + back * old[...].astype(F32)
    image_out[...] = image
    inner_0 = over_rows(r0 * image)
    inner_1 = over_rows(r1 * image)
    norm_1 = over_rows(r1 * r1)
    cross = over_rows(r0 * r1)
    own_1 = ratio(inner_1, norm_1)
    rest = image - own_1 * r1
    own_0 = ratio(over_rows(r0 * rest), over_rows(r0 * r0))
    message_of(message, rest - own_0 * r0, [own_0, own_1], [inner_0, inner_1, norm_1, cross])
    coefs[...] = pack_rows([taken, scale_0], 8)


def third_kernel(bands, damping, r_0, r_1, image_1, coefs, *refs):
    first = refs[:bands]
    second = refs[bands : 2 * bands]
    parts = refs[2 * bands : 3 * bands]
    r_2_out, image_out, sums_out, coefs_out = refs[3 * bands :]
    width = r_0.shape[0]
    inner_0, inner_1, norm_1, cross = global_sums(parts, width, 2, 4)
    taken_00 = coefs[0:1, :]
    scale_0 = coefs[1:2, :]
    scale_1 = norm_1 + EPS * scale_0
    taken_0 = inner_0 / scale_0
    taken_1 = (inner_1 - taken_0 * cross) / scale_1
    r0 = r_0[...]
    r1 = r_1[...]
    r2 = image_1[...] - taken_0 * r0 - taken_1 * r1
    r_2_out[...] = r2
    image = damping[...] * r2
    for old_0, old_1, part in zip(first, second, parts):
        back_0 = part[width : width + 1, :].astype(F32) - taken_0
        back_1 = part[width + 1 : width + 2, :].astype(F32) - taken_1
        back_0 = back_0 + back_1 * (old_1[width : width + 1, :].astype(F32) - taken_00)
        image = image + part[:width, :].astype(F32)
        image = image + back_1 * old_1[:width, :].astype(F32) + back_0 * old_0[...].astype(F32)
    image_out[...] = image
    pairs = ((r0, image), (r1, image), (r2, image), (r2, r2), (image, image), (r0, r2), (r1, r2))
    sums_out[...] = pack_rows([over_rows(a * b) for a, b in pairs], 8)
    coefs_out[...] = pack_rows([taken_00, taken_0, taken_1, scale_0, scale_1, cross, norm_1], 8)


def last_kernel(rescale, coefs, sums, r_0, r_1, r_2, image_2, basis_out, hessenberg_out, basis, hessenberg, sems):
    total = sums[0]
    for k in range(1, sums.shape[0]):
        total = total + sums[k]
    inner_0, inner_1, inner_2, norm_2, square, cross_02, cross_12 = [row_of(total, i) for i in range(7)]
    taken_00, taken_01, taken_11, scale_0, scale_1, cross_01, norm_1 = [coefs[i : i + 1, :] for i in range(7)]
    norm_0 = scale_0 - EPS
    scale_2 = norm_2 + EPS * scale_1
    taken_0 = inner_0 / scale_0
    taken_1 = (inner_1 - taken_0 * cross_01) / scale_1
    taken_2 = (inner_2 - taken_0 * cross_02 - taken_1 * cross_12) / scale_2
    square = square - taken_0 * (2.0 * inner_0 - taken_0 * norm_0)
    square = square - taken_1 * (2.0 * (inner_1 - taken_0 * cross_01) - taken_1 * norm_1)
    square = square - taken_2 * (2.0 * (inner_2 - taken_0 * cross_02 - taken_1 * cross_12) - taken_2 * norm_2)
    scale_3 = jnp.maximum(square, 0.0) + EPS * scale_2
    inverse = [lax.rsqrt(scale) for scale in (scale_0, scale_1, scale_2, scale_3)]
    root = [scale * inv for scale, inv in zip((scale_0, scale_1, scale_2, scale_3), inverse)]
    moves = [pltpu.make_async_copy(basis.at[i], basis_out.at[i], sems.at[i]) for i in range(ITERS + 1)]
    moves.append(pltpu.make_async_copy(hessenberg, hessenberg_out, sems.at[ITERS + 1]))
    for i, vector in enumerate((r_0, r_1, r_2)):
        basis[i] = vector[...] * (inverse[i] * rescale)
        moves[i].start()
    image = image_2[...] - taken_0 * r_0[...] - taken_1 * r_1[...] - taken_2 * r_2[...]
    basis[3] = image * (inverse[3] * rescale)
    moves[3].start()
    hessenberg[...] = jnp.zeros(hessenberg.shape, F32)
    for step, column in enumerate(((taken_00,), (taken_01, taken_11), (taken_0, taken_1, taken_2))):
        for i, taken in enumerate(column):
            hessenberg[step, i : i + 1, :] = taken * root[i] * inverse[step]
        hessenberg[step, step + 1 : step + 2, :] = root[step + 1] * inverse[step]
    moves[4].start()
    for move in moves:
        move.wait()


def call(kernel, outs, *operands, scalars=0, scratch=()):
    vmem = pl.BlockSpec(memory_space=pltpu.VMEM)
    smem = pl.BlockSpec(memory_space=pltpu.SMEM)
    spaces = [pltpu.SMEM] * scalars + [pltpu.VMEM] * (len(operands) - scalars)
    operands = [pltpu.with_memory_space_constraint(x, space) for x, space in zip(operands, spaces)]
    return pl.pallas_call(
        kernel,
        out_shape=[pltpu.VMEM(shape, dtype) for shape, dtype in outs],
        in_specs=[smem] * scalars + [vmem] * (len(operands) - scalars),
        out_specs=[vmem] * len(outs),
        scratch_shapes=list(scratch),
        compiler_params=pltpu.CompilerParams(vmem_limit_bytes=VMEM_LIMIT),
    )(*operands)


def gather(message, shards, aside=None):
    blocks = [None] * shards
    blocks[0] = message
    for k in range(2, shards, 2):
        blocks[k] = lax.ppermute(message, "rows", partners(shards, k))
    if aside is not None:
        *blocks[2::2], aside = lax.optimization_barrier((*blocks[2::2], aside))
    for k in range(0, shards, 2):
        blocks[k + 1] = lax.ppermute(blocks[k], "rows", partners(shards, 1))
    return blocks, aside


def on_device(tiles, tile_row, tile_col, tile_count, damping, right_side):
    bands = lax.axis_size("band")
    shards = lax.axis_size("rows")
    slots = tiles.shape[2]
    width = right_side.shape[0]
    queries = right_side.shape[1]
    rescale = math.sqrt(width * bands * shards)
    damping = damping.reshape(1, queries)
    block = ((width, queries), F32)
    long_message = ((width + EXTRA, queries), BF16)
    small = ((8, queries), F32)

    def multiply(step, blocks, *older):
        extra = EXTRA if step else 0
        outs = [((width + extra, queries), F32)] + [((width + extra, queries), BF16)] * (bands - 1)
        if step < ITERS - 1:
            outs.append(((slots, width, queries), F32))
        if step == 1:
            outs.append(((slots + 8 - slots % 8, queries), F32))
        results = call(
            functools.partial(product_kernel, step, shards, bands, slots, width),
            outs,
            plan,
            staged,
            *blocks,
            *older,
            scalars=1,
            scratch=(
                pltpu.VMEM((width, queries), BF16),
                pltpu.VMEM((shards, EXTRA, queries), F32),
                pltpu.VMEM((bands, width, queries), F32),
            ),
        )
        parts = [results[0]] + [lax.ppermute(results[k], "band", partners(bands, k)) for k in reversed(range(1, bands))]
        return parts, list(results[bands:])

    smem = pl.BlockSpec(memory_space=pltpu.SMEM)
    vmem = pl.BlockSpec(memory_space=pltpu.VMEM)
    hbm = pl.BlockSpec(memory_space=pltpu.HBM)
    params = pltpu.CompilerParams(vmem_limit_bytes=VMEM_LIMIT)
    right_side, message = pl.pallas_call(
        open_kernel,
        out_shape=[pltpu.VMEM((width, queries), F32), pltpu.VMEM((width, queries), BF16)],
        in_specs=[hbm],
        out_specs=[vmem] * 2,
        scratch_shapes=[pltpu.SemaphoreType.DMA(())],
        compiler_params=params,
    )(pltpu.with_memory_space_constraint(right_side, pltpu.HBM))
    staged, plan = pl.pallas_call(
        stage_kernel,
        out_shape=[pltpu.VMEM(tiles.shape[2:], BF16), pltpu.SMEM((1, 1 + 2 * slots), jnp.int32)],
        in_specs=[hbm] * 3 + [smem, vmem],
        out_specs=[vmem, smem],
        scratch_shapes=[
            pltpu.SMEM(tile_row.shape, jnp.int32),
            pltpu.SMEM(tile_col.shape, jnp.int32),
            pltpu.SemaphoreType.DMA((3,)),
        ],
        compiler_params=params,
    )(
        *[pltpu.with_memory_space_constraint(x, pltpu.HBM) for x in (tiles, tile_row, tile_col)],
        tile_count,
        pltpu.with_memory_space_constraint(message, pltpu.VMEM),
    )
    blocks, (staged, plan) = gather(message, shards, (staged, plan))
    parts_0, (stored_0,) = multiply(0, blocks)
    image_0, message = call(functools.partial(first_kernel, bands), [block, long_message], damping, right_side, *parts_0)
    parts_1, (stored_1, side) = multiply(1, gather(message, shards)[0], stored_0)
    r_1, image_1, message, coefs = call(
        functools.partial(second_kernel, bands), [block, block, long_message, small], damping, right_side, image_0, *parts_0, *parts_1
    )
    parts_2, _ = multiply(2, gather(message, shards)[0], stored_0, stored_1, side, coefs)
    r_2, image_2, sums, coefs = call(
        functools.partial(third_kernel, bands),
        [block, block, small, small],
        damping,
        right_side,
        r_1,
        image_1,
        coefs,
        *parts_0,
        *parts_1,
        *parts_2,
    )
    everyone = jnp.broadcast_to(sums[None], (bands * shards, *sums.shape))
    everyone = lax.all_to_all(everyone, ("rows", "band"), 0, 0, tiled=True)
    shapes = ((ITERS + 1, width, queries), (ITERS, ITERS + 1, queries))
    basis, hessenberg = pl.pallas_call(
        functools.partial(last_kernel, rescale),
        out_shape=[jax.ShapeDtypeStruct(shape, F32) for shape in shapes],
        in_specs=[vmem] * 6,
        out_specs=[pl.BlockSpec(memory_space=pltpu.HBM)] * 2,
        scratch_shapes=[pltpu.VMEM(shape, F32) for shape in shapes] + [pltpu.SemaphoreType.DMA((ITERS + 2,))],
        compiler_params=pltpu.CompilerParams(vmem_limit_bytes=VMEM_LIMIT),
    )(*[pltpu.with_memory_space_constraint(x, pltpu.VMEM) for x in (coefs, everyone, right_side, r_1, r_2, image_2)])
    return basis, jnp.swapaxes(hessenberg, 0, 1)


def solution(mesh):
    return jax.shard_map(
        lambda *args: tuple(on_device(*args)),
        mesh=mesh,
        in_specs=(
            P("rows", "band", None, None, None),
            P("rows", "band", None),
            P("rows", "band", None),
            P("rows", "band"),
            P(),
            P(("rows", "band"), None),
        ),
        out_specs=(P(None, ("rows", "band"), None), P()),
        check_vma=False,
    )
```

```python
import functools
import math

import jax
import jax.numpy as jnp
from jax import lax
from jax.experimental import pallas as pl
from jax.experimental.pallas import tpu as pltpu
from jax.sharding import PartitionSpec as P

ITERS = 3
EPS = 1e-06
EXTRA = (0, 8, 16)
VMEM_LIMIT = 16 << 20
LATE = (3, 5)
F32 = jnp.float32
BF16 = jnp.bfloat16


def partners(size, step):
    return [(i, i ^ step) for i in range(size)]


def pieces(value):
    high = value.astype(BF16).astype(F32)
    rest = value - high
    middle = rest.astype(BF16).astype(F32)
    return [high, middle, rest - middle]


def pack_rows(rows, count):
    place = lax.broadcasted_iota(jnp.int32, (count, rows[0].shape[1]), 0)
    packed = jnp.zeros(place.shape, F32)
    for index, row in enumerate(rows):
        packed = jnp.where(place == index, row, packed)
    return packed


def row_of(packed, index):
    return packed[index : index + 1, :]


def sum_of(packed, index):
    return row_of(packed, index) + row_of(packed, index + 1) + row_of(packed, index + 2)


def ratio(top, bottom):
    safe = jnp.where(bottom > 0, bottom, 1.0)
    return jnp.where(bottom > 0, top / safe, 0.0).astype(BF16).astype(F32)


def over_rows(value):
    return jnp.sum(value, axis=0, keepdims=True)


def open_kernel(right_side, r_0, message, sems):
    rows = right_side.shape[0] // sems.shape[0]
    spans = [pl.ds(i * rows, rows) for i in range(sems.shape[0])]
    moves = [pltpu.make_async_copy(right_side.at[span], r_0.at[span], sems.at[i]) for i, span in enumerate(spans)]
    for move in moves:
        move.start()
    for span, move in zip(spans, moves):
        move.wait()
        message[span, :] = r_0[span, :].astype(BF16)


def stage_kernel(tiles, row, col, count, after, staged, plan, rows, cols, sems):
    del after
    slots = row.shape[2]
    pairs = ((row, rows), (col, cols), (tiles.at[0, 0], staged))
    moves = [pltpu.make_async_copy(source, target, sems.at[i]) for i, (source, target) in enumerate(pairs)]
    for move in moves:
        move.start()
    for move in moves[:2]:
        move.wait()
    plan[0, 0] = count[0, 0]
    shard = lax.axis_index("rows")
    band = lax.axis_index("band")
    for slot in range(slots):
        plan[0, 1 + slot] = cols[0, 0, slot] ^ shard
        plan[0, 1 + slots + slot] = rows[0, 0, slot] ^ band
    moves[2].wait()


def early_kernel(late, plan, tiles, *refs):
    *blocks, stored, column = refs
    slots, width, _ = stored.shape
    numbers = [k for k in range(len(blocks) + len(late)) if k not in late]
    for slot in range(slots):
        source = plan[0, 1 + slot]

        wait = functools.reduce(jnp.logical_or, [source == k for k in late])

        @pl.when((slot < plan[0, 0]) & jnp.logical_not(wait))
        def _(slot=slot, source=source):
            for k, block in zip(numbers, blocks):

                @pl.when(source == k)
                def _(block=block):
                    column[...] = block[:width, :]

            stored[slot] = jnp.dot(tiles[slot], column[...], preferred_element_type=F32)


def product_kernel(step, late, shards, bands, slots, width, *refs):
    refs = list(refs)
    take = lambda n: [refs.pop(0) for _ in range(n)]
    plan, tiles, early = take(3)
    blocks = take(shards)
    older = take(step)
    side, coefs = take(2) if step == 2 else (None, None)
    stored = take(1)[0]
    outs = take(bands)
    side_out = take(1)[0] if step == 1 else None
    extras, total = take(2)
    del early
    total[...] = jnp.zeros(total.shape, F32)
    rows = []
    wholes = []
    if step:
        for k in range(shards):
            extras[k] = blocks[k][width:, :].astype(F32)
        added = extras[0]
        for k in range(1, shards):
            added = added + extras[k]
        sums = [sum_of(added, step + 3 * i) for i in range(2 if step == 1 else 4)]
        if step == 1:
            wholes = [ratio(sums[0], sums[1])]
        else:
            inner_0, inner_1, norm_1, cross = sums
            whole_1 = ratio(inner_1, norm_1)
            wholes = [ratio(inner_0 - whole_1 * cross, side[slots : slots + 1, :]), whole_1]
        rows = wholes + [piece for value in sums for piece in pieces(value)]
    if side_out is not None:
        side_out[...] = jnp.zeros(side_out.shape, F32)
        side_out[slots : slots + 1, :] = sums[1]
    for slot in range(slots):

        @pl.when(slot < plan[0, 0])
        def _(slot=slot):
            source = plan[0, 1 + slot]
            target = plan[0, 1 + slots + slot]

            for k in late:

                @pl.when(source == k)
                def _(k=k):
                    stored[slot] = jnp.dot(tiles[slot], blocks[k][:width, :], preferred_element_type=F32)

            product = stored[slot]
            if step:
                extra = extras[source]
                if step == 1:
                    own = row_of(extra, 0)
                    side_out[slot : slot + 1, :] = own
                    product = product + (own - wholes[0]) * older[0][slot]
                else:
                    first = row_of(extra, 0) - wholes[0]
                    second = row_of(extra, 1) - wholes[1]
                    first = first + second * (side[slot : slot + 1, :] - coefs[0:1, :])
                    product = product + second * older[1][slot] + first * older[0][slot]
            total[target] += product

    outs[0][:width, :] = total[0]
    for k in range(1, bands):
        outs[k][:width, :] = total[k].astype(BF16)
    if step:
        packed = pack_rows(rows, EXTRA[step])
        outs[0][width:, :] = packed
        for k in range(1, bands):
            outs[k][width:, :] = packed.astype(BF16)


def message_of(message, value, coefs, sums):
    width = value.shape[0]
    message[:width, :] = value.astype(BF16)
    rows = coefs + [piece for entry in sums for piece in pieces(entry)]
    message[width:, :] = pack_rows(rows, message.shape[0] - width).astype(BF16)


def first_kernel(bands, damping, r_0, *refs):
    parts = refs[:bands]
    image_out, message = refs[bands:]
    r = r_0[...]
    image = damping[...] * r
    for part in parts:
        image = image + part[...].astype(F32)
    image_out[...] = image
    inner = over_rows(r * image)
    norm = over_rows(r * r)
    own = ratio(inner, norm)
    message_of(message, image - own * r, [own], [inner, norm])


def global_sums(parts, width, step, count):
    packed = parts[0][width:, :].astype(F32)
    for part in parts[1:]:
        packed = packed + part[width:, :].astype(F32)
    return [sum_of(packed, step + 3 * i) for i in range(count)]


def second_kernel(bands, damping, r_0, image_0, *refs):
    first = refs[:bands]
    parts = refs[bands : 2 * bands]
    r_1_out, image_out, message, coefs = refs[2 * bands :]
    width = r_0.shape[0]
    inner, norm = global_sums(parts, width, 1, 2)
    scale_0 = norm + EPS
    taken = inner / scale_0
    r0 = r_0[...]
    r1 = image_0[...] - taken * r0
    r_1_out[...] = r1
    image = damping[...] * r1
    for old, part in zip(first, parts):
        back = part[width : width + 1, :].astype(F32) - taken
        image = image + part[:width, :].astype(F32) + back * old[...].astype(F32)
    image_out[...] = image
    inner_0 = over_rows(r0 * image)
    inner_1 = over_rows(r1 * image)
    norm_1 = over_rows(r1 * r1)
    cross = over_rows(r0 * r1)
    own_1 = ratio(inner_1, norm_1)
    rest = image - own_1 * r1
    own_0 = ratio(over_rows(r0 * rest), over_rows(r0 * r0))
    message_of(message, rest - own_0 * r0, [own_0, own_1], [inner_0, inner_1, norm_1, cross])
    coefs[...] = pack_rows([taken, scale_0], 8)


def third_kernel(bands, damping, r_0, r_1, image_1, coefs, *refs):
    first = refs[:bands]
    second = refs[bands : 2 * bands]
    parts = refs[2 * bands : 3 * bands]
    r_2_out, image_out, sums_out, coefs_out = refs[3 * bands :]
    width = r_0.shape[0]
    inner_0, inner_1, norm_1, cross = global_sums(parts, width, 2, 4)
    taken_00 = coefs[0:1, :]
    scale_0 = coefs[1:2, :]
    scale_1 = norm_1 + EPS * scale_0
    taken_0 = inner_0 / scale_0
    taken_1 = (inner_1 - taken_0 * cross) / scale_1
    r0 = r_0[...]
    r1 = r_1[...]
    r2 = image_1[...] - taken_0 * r0 - taken_1 * r1
    r_2_out[...] = r2
    image = damping[...] * r2
    for old_0, old_1, part in zip(first, second, parts):
        back_0 = part[width : width + 1, :].astype(F32) - taken_0
        back_1 = part[width + 1 : width + 2, :].astype(F32) - taken_1
        back_0 = back_0 + back_1 * (old_1[width : width + 1, :].astype(F32) - taken_00)
        image = image + part[:width, :].astype(F32)
        image = image + back_1 * old_1[:width, :].astype(F32) + back_0 * old_0[...].astype(F32)
    image_out[...] = image
    pairs = ((r0, image), (r1, image), (r2, image), (r2, r2), (image, image), (r0, r2), (r1, r2))
    sums_out[...] = pack_rows([over_rows(a * b) for a, b in pairs], 8)
    coefs_out[...] = pack_rows([taken_00, taken_0, taken_1, scale_0, scale_1, cross, norm_1], 8)


def last_kernel(rescale, coefs, sums, r_0, r_1, r_2, image_2, basis_out, hessenberg_out, basis, hessenberg, sems):
    moves = [pltpu.make_async_copy(basis.at[i], basis_out.at[i], sems.at[i]) for i in range(ITERS + 1)]
    moves.append(pltpu.make_async_copy(hessenberg, hessenberg_out, sems.at[ITERS + 1]))

    def put(i, value, scale):
        basis[i] = value * (lax.rsqrt(scale) * rescale)
        moves[i].start()

    taken_00, taken_01, taken_11, scale_0, scale_1, cross_01, norm_1 = [coefs[i : i + 1, :] for i in range(7)]
    put(0, r_0[...], scale_0)
    put(1, r_1[...], scale_1)
    total = jnp.sum(sums[...], axis=0)
    inner_0, inner_1, inner_2, norm_2, square, cross_02, cross_12 = [row_of(total, i) for i in range(7)]
    scale_2 = norm_2 + EPS * scale_1
    put(2, r_2[...], scale_2)
    norm_0 = scale_0 - EPS
    taken_0 = inner_0 / scale_0
    inner_1 = inner_1 - taken_0 * cross_01
    taken_1 = inner_1 / scale_1
    inner_2 = inner_2 - taken_0 * cross_02 - taken_1 * cross_12
    taken_2 = inner_2 / scale_2
    square = square - taken_0 * (2.0 * inner_0 - taken_0 * norm_0)
    square = square - taken_1 * (2.0 * inner_1 - taken_1 * norm_1)
    square = square - taken_2 * (2.0 * inner_2 - taken_2 * norm_2)
    scale_3 = jnp.maximum(square, 0.0) + EPS * scale_2
    put(3, image_2[...] - taken_0 * r_0[...] - taken_1 * r_1[...] - taken_2 * r_2[...], scale_3)
    scales = (scale_0, scale_1, scale_2, scale_3)
    inverse = [lax.rsqrt(scale) for scale in scales]
    root = [scale * inv for scale, inv in zip(scales, inverse)]
    hessenberg[...] = jnp.zeros(hessenberg.shape, F32)
    for step, column in enumerate(((taken_00,), (taken_01, taken_11), (taken_0, taken_1, taken_2))):
        for i, taken in enumerate(column):
            hessenberg[step, i : i + 1, :] = taken * root[i] * inverse[step]
        hessenberg[step, step + 1 : step + 2, :] = root[step + 1] * inverse[step]
    moves[ITERS + 1].start()
    for move in moves:
        move.wait()


def call(kernel, outs, *operands, scalars=0, scratch=(), aliases=None):
    vmem = pl.BlockSpec(memory_space=pltpu.VMEM)
    smem = pl.BlockSpec(memory_space=pltpu.SMEM)
    spaces = [pltpu.SMEM] * scalars + [pltpu.VMEM] * (len(operands) - scalars)
    operands = [pltpu.with_memory_space_constraint(x, space) for x, space in zip(operands, spaces)]
    return pl.pallas_call(
        kernel,
        out_shape=[pltpu.VMEM(shape, dtype) for shape, dtype in outs],
        in_specs=[smem] * scalars + [vmem] * (len(operands) - scalars),
        out_specs=[vmem] * len(outs),
        scratch_shapes=list(scratch),
        input_output_aliases=aliases or {},
        compiler_params=pltpu.CompilerParams(vmem_limit_bytes=VMEM_LIMIT),
    )(*operands)


def gather(message, shards, aside=None):
    blocks = [None] * shards
    blocks[0] = message
    for k in range(2, shards, 2):
        blocks[k] = lax.ppermute(message, "rows", partners(shards, k))
    if aside is not None:
        *blocks[2::2], aside = lax.optimization_barrier((*blocks[2::2], aside))
    for k in range(0, shards, 2):
        blocks[k + 1] = lax.ppermute(blocks[k], "rows", partners(shards, 1))
    return blocks, aside


def on_device(tiles, tile_row, tile_col, tile_count, damping, right_side):
    bands = lax.axis_size("band")
    shards = lax.axis_size("rows")
    slots = tiles.shape[2]
    width = right_side.shape[0]
    queries = right_side.shape[1]
    rescale = math.sqrt(width * bands * shards)
    damping = damping.reshape(1, queries)
    block = ((width, queries), F32)
    small = ((8, queries), F32)

    def message_shape(step):
        return (width + EXTRA[step], queries), BF16

    def multiply(step, blocks, *older):
        product = ((slots, width, queries), F32)
        (early,) = call(
            functools.partial(early_kernel, LATE),
            [product],
            plan,
            staged,
            *[block for k, block in enumerate(blocks) if k not in LATE],
            scalars=1,
            scratch=(pltpu.VMEM((width, queries), BF16),),
        )
        outs = [product, ((width + EXTRA[step], queries), F32)] + [message_shape(step)] * (bands - 1)
        if step == 1:
            outs.append(((slots + 8 - slots % 8, queries), F32))
        stored, *results = call(
            functools.partial(product_kernel, step, LATE, shards, bands, slots, width),
            outs,
            plan,
            staged,
            early,
            *blocks,
            *older,
            scalars=1,
            scratch=(pltpu.VMEM((shards, max(EXTRA[step], 8), queries), F32), pltpu.VMEM((bands, width, queries), F32)),
            aliases={2: 0},
        )
        parts = [results[0]] + [lax.ppermute(results[k], "band", partners(bands, k)) for k in reversed(range(1, bands))]
        return parts, [stored, *results[bands:]]

    smem = pl.BlockSpec(memory_space=pltpu.SMEM)
    vmem = pl.BlockSpec(memory_space=pltpu.VMEM)
    hbm = pl.BlockSpec(memory_space=pltpu.HBM)
    params = pltpu.CompilerParams(vmem_limit_bytes=VMEM_LIMIT)
    right_side, message = pl.pallas_call(
        open_kernel,
        out_shape=[pltpu.VMEM((width, queries), F32), pltpu.VMEM((width, queries), BF16)],
        in_specs=[hbm],
        out_specs=[vmem] * 2,
        scratch_shapes=[pltpu.SemaphoreType.DMA((4,))],
        compiler_params=params,
    )(pltpu.with_memory_space_constraint(right_side, pltpu.HBM))
    staged, plan = pl.pallas_call(
        stage_kernel,
        out_shape=[pltpu.VMEM(tiles.shape[2:], BF16), pltpu.SMEM((1, 1 + 2 * slots), jnp.int32)],
        in_specs=[hbm] * 3 + [smem, vmem],
        out_specs=[vmem, smem],
        scratch_shapes=[
            pltpu.SMEM(tile_row.shape, jnp.int32),
            pltpu.SMEM(tile_col.shape, jnp.int32),
            pltpu.SemaphoreType.DMA((3,)),
        ],
        compiler_params=params,
    )(
        *[pltpu.with_memory_space_constraint(x, pltpu.HBM) for x in (tiles, tile_row, tile_col)],
        tile_count,
        pltpu.with_memory_space_constraint(message, pltpu.VMEM),
    )
    blocks, (staged, plan) = gather(message, shards, (staged, plan))
    parts_0, (stored_0,) = multiply(0, blocks)
    image_0, message = call(functools.partial(first_kernel, bands), [block, message_shape(1)], damping, right_side, *parts_0)
    parts_1, (stored_1, side) = multiply(1, gather(message, shards)[0], stored_0)
    r_1, image_1, message, coefs = call(
        functools.partial(second_kernel, bands), [block, block, message_shape(2), small], damping, right_side, image_0, *parts_0, *parts_1
    )
    parts_2, _ = multiply(2, gather(message, shards)[0], stored_0, stored_1, side, coefs)
    r_2, image_2, sums, coefs = call(
        functools.partial(third_kernel, bands),
        [block, block, small, small],
        damping,
        right_side,
        r_1,
        image_1,
        coefs,
        *parts_0,
        *parts_1,
        *parts_2,
    )
    everyone = jnp.broadcast_to(sums[None], (bands * shards, *sums.shape))
    everyone = lax.all_to_all(everyone, ("rows", "band"), 0, 0, tiled=True)
    shapes = ((ITERS + 1, width, queries), (ITERS, ITERS + 1, queries))
    basis, hessenberg = pl.pallas_call(
        functools.partial(last_kernel, rescale),
        out_shape=[jax.ShapeDtypeStruct(shape, F32) for shape in shapes],
        in_specs=[vmem] * 6,
        out_specs=[pl.BlockSpec(memory_space=pltpu.HBM)] * 2,
        scratch_shapes=[pltpu.VMEM(shape, F32) for shape in shapes] + [pltpu.SemaphoreType.DMA((ITERS + 2,))],
        compiler_params=pltpu.CompilerParams(vmem_limit_bytes=VMEM_LIMIT),
    )(*[pltpu.with_memory_space_constraint(x, pltpu.VMEM) for x in (coefs, everyone, right_side, r_1, r_2, image_2)])
    return basis, jnp.swapaxes(hessenberg, 0, 1)


def solution(mesh):
    return jax.shard_map(
        lambda *args: tuple(on_device(*args)),
        mesh=mesh,
        in_specs=(
            P("rows", "band", None, None, None),
            P("rows", "band", None),
            P("rows", "band", None),
            P("rows", "band"),
            P(),
            P(("rows", "band"), None),
        ),
        out_specs=(P(None, ("rows", "band"), None), P()),
        check_vma=False,
    )
```

```python
import functools
import math

import jax
import jax.numpy as jnp
from jax import lax
from jax.experimental import pallas as pl
from jax.experimental.pallas import tpu as pltpu
from jax.sharding import PartitionSpec as P

ITERS = 3
EPS = 1e-06
EXTRA = (0, 8, 16)
VMEM_LIMIT = 16 << 20
LATE = (3, 5)
F32 = jnp.float32
BF16 = jnp.bfloat16


def partners(size, step):
    return [(i, i ^ step) for i in range(size)]


def pieces(value):
    high = value.astype(BF16).astype(F32)
    rest = value - high
    middle = rest.astype(BF16).astype(F32)
    return [high, middle, rest - middle]


def pack_rows(rows, count):
    place = lax.broadcasted_iota(jnp.int32, (count, rows[0].shape[1]), 0)
    packed = jnp.zeros(place.shape, F32)
    for index, row in enumerate(rows):
        packed = jnp.where(place == index, row, packed)
    return packed


def row_of(packed, index):
    return packed[index : index + 1, :]


def sum_of(packed, index):
    return row_of(packed, index) + row_of(packed, index + 1) + row_of(packed, index + 2)


def ratio(top, bottom):
    safe = jnp.where(bottom > 0, bottom, 1.0)
    return jnp.where(bottom > 0, top / safe, 0.0).astype(BF16).astype(F32)


def over_rows(value):
    return jnp.sum(value, axis=0, keepdims=True)


def open_kernel(right_side, r_0, message, sems):
    rows = right_side.shape[0] // sems.shape[0]
    spans = [pl.ds(i * rows, rows) for i in range(sems.shape[0])]
    moves = [pltpu.make_async_copy(right_side.at[span], r_0.at[span], sems.at[i]) for i, span in enumerate(spans)]
    for move in moves:
        move.start()
    for span, move in zip(spans, moves):
        move.wait()
        message[span, :] = r_0[span, :].astype(BF16)


def stage_kernel(tiles, row, col, count, after, staged, plan, rows, cols, sems):
    del after
    slots = row.shape[2]
    pairs = ((row, rows), (col, cols), (tiles.at[0, 0], staged))
    moves = [pltpu.make_async_copy(source, target, sems.at[i]) for i, (source, target) in enumerate(pairs)]
    for move in moves:
        move.start()
    for move in moves[:2]:
        move.wait()
    plan[0, 0] = count[0, 0]
    shard = lax.axis_index("rows")
    band = lax.axis_index("band")
    for slot in range(slots):
        plan[0, 1 + slot] = cols[0, 0, slot] ^ shard
        plan[0, 1 + slots + slot] = rows[0, 0, slot] ^ band
    moves[2].wait()


def early_kernel(late, plan, tiles, *refs):
    *blocks, stored, column = refs
    slots, width, _ = stored.shape
    numbers = [k for k in range(len(blocks) + len(late)) if k not in late]
    for slot in range(slots):
        source = plan[0, 1 + slot]

        wait = functools.reduce(jnp.logical_or, [source == k for k in late])

        @pl.when((slot < plan[0, 0]) & jnp.logical_not(wait))
        def _(slot=slot, source=source):
            for k, block in zip(numbers, blocks):

                @pl.when(source == k)
                def _(block=block):
                    column[...] = block[:width, :]

            stored[slot] = jnp.dot(tiles[slot], column[...], preferred_element_type=F32)


def product_kernel(step, late, shards, bands, slots, width, *refs):
    refs = list(refs)
    take = lambda n: [refs.pop(0) for _ in range(n)]
    plan, tiles, early = take(3)
    blocks = take(shards)
    older = take(step)
    side, coefs = take(2) if step == 2 else (None, None)
    stored = take(1)[0]
    outs = take(bands)
    side_out = take(1)[0] if step == 1 else None
    extras, total = take(2)
    del early
    total[...] = jnp.zeros(total.shape, F32)
    rows = []
    wholes = []
    if step:
        for k in range(shards):
            extras[k] = blocks[k][width:, :].astype(F32)
        added = extras[0]
        for k in range(1, shards):
            added = added + extras[k]
        sums = [sum_of(added, step + 3 * i) for i in range(2 if step == 1 else 4)]
        if step == 1:
            wholes = [ratio(sums[0], sums[1])]
        else:
            inner_0, inner_1, norm_1, cross = sums
            whole_1 = ratio(inner_1, norm_1)
            wholes = [ratio(inner_0 - whole_1 * cross, side[slots : slots + 1, :]), whole_1]
        rows = wholes + [piece for value in sums for piece in pieces(value)]
    if side_out is not None:
        side_out[...] = jnp.zeros(side_out.shape, F32)
        side_out[slots : slots + 1, :] = sums[1]
    for slot in range(slots):

        @pl.when(slot < plan[0, 0])
        def _(slot=slot):
            source = plan[0, 1 + slot]
            target = plan[0, 1 + slots + slot]

            for k in late:

                @pl.when(source == k)
                def _(k=k):
                    stored[slot] = jnp.dot(tiles[slot], blocks[k][:width, :], preferred_element_type=F32)

            product = stored[slot]
            if step:
                extra = extras[source]
                if step == 1:
                    own = row_of(extra, 0)
                    side_out[slot : slot + 1, :] = own
                    product = product + (own - wholes[0]) * older[0][slot]
                else:
                    first = row_of(extra, 0) - wholes[0]
                    second = row_of(extra, 1) - wholes[1]
                    first = first + second * (side[slot : slot + 1, :] - coefs[0:1, :])
                    product = product + second * older[1][slot] + first * older[0][slot]
            total[target] += product

    outs[0][:width, :] = total[0]
    for k in range(1, bands):
        outs[k][:width, :] = total[k].astype(BF16)
    if step:
        packed = pack_rows(rows, EXTRA[step])
        outs[0][width:, :] = packed
        for k in range(1, bands):
            outs[k][width:, :] = packed.astype(BF16)


def message_of(message, value, coefs, sums):
    width = value.shape[0]
    message[:width, :] = value.astype(BF16)
    rows = coefs + [piece for entry in sums for piece in pieces(entry)]
    message[width:, :] = pack_rows(rows, message.shape[0] - width).astype(BF16)


def first_kernel(bands, damping, r_0, *refs):
    parts = refs[:bands]
    image_out, message = refs[bands:]
    r = r_0[...]
    image = damping[...] * r
    for part in parts:
        image = image + part[...].astype(F32)
    image_out[...] = image
    inner = over_rows(r * image)
    norm = over_rows(r * r)
    own = ratio(inner, norm)
    message_of(message, image - own * r, [own], [inner, norm])


def global_sums(parts, width, step, count):
    packed = parts[0][width:, :].astype(F32)
    for part in parts[1:]:
        packed = packed + part[width:, :].astype(F32)
    return [sum_of(packed, step + 3 * i) for i in range(count)]


def second_kernel(bands, damping, r_0, image_0, *refs):
    first = refs[:bands]
    parts = refs[bands : 2 * bands]
    r_1_out, image_out, message, coefs = refs[2 * bands :]
    width = r_0.shape[0]
    inner, norm = global_sums(parts, width, 1, 2)
    scale_0 = norm + EPS
    taken = inner / scale_0
    r0 = r_0[...]
    r1 = image_0[...] - taken * r0
    r_1_out[...] = r1
    image = damping[...] * r1
    for old, part in zip(first, parts):
        back = part[width : width + 1, :].astype(F32) - taken
        image = image + part[:width, :].astype(F32) + back * old[...].astype(F32)
    image_out[...] = image
    inner_0 = over_rows(r0 * image)
    inner_1 = over_rows(r1 * image)
    norm_1 = over_rows(r1 * r1)
    cross = over_rows(r0 * r1)
    own_1 = ratio(inner_1, norm_1)
    rest = image - own_1 * r1
    own_0 = ratio(over_rows(r0 * rest), over_rows(r0 * r0))
    message_of(message, rest - own_0 * r0, [own_0, own_1], [inner_0, inner_1, norm_1, cross])
    coefs[...] = pack_rows([taken, scale_0], 8)


def third_kernel(bands, damping, r_0, r_1, image_1, coefs, *refs):
    first = refs[:bands]
    second = refs[bands : 2 * bands]
    parts = refs[2 * bands : 3 * bands]
    r_2_out, image_out, sums_out, coefs_out = refs[3 * bands :]
    width = r_0.shape[0]
    inner_0, inner_1, norm_1, cross = global_sums(parts, width, 2, 4)
    taken_00 = coefs[0:1, :]
    scale_0 = coefs[1:2, :]
    scale_1 = norm_1 + EPS * scale_0
    taken_0 = inner_0 / scale_0
    taken_1 = (inner_1 - taken_0 * cross) / scale_1
    r0 = r_0[...]
    r1 = r_1[...]
    r2 = image_1[...] - taken_0 * r0 - taken_1 * r1
    r_2_out[...] = r2
    image = damping[...] * r2
    for old_0, old_1, part in zip(first, second, parts):
        back_0 = part[width : width + 1, :].astype(F32) - taken_0
        back_1 = part[width + 1 : width + 2, :].astype(F32) - taken_1
        back_0 = back_0 + back_1 * (old_1[width : width + 1, :].astype(F32) - taken_00)
        image = image + part[:width, :].astype(F32)
        image = image + back_1 * old_1[:width, :].astype(F32) + back_0 * old_0[...].astype(F32)
    image_out[...] = image
    queries = r0.shape[1]
    for i, (a, b) in enumerate(((r0, image), (r1, image), (r2, image), (r2, r2), (image, image))):
        sums_out[:, i * queries : (i + 1) * queries] = over_rows(a * b)
    coefs_out[...] = pack_rows([taken_00, taken_0, taken_1, scale_0, scale_1, cross, norm_1], 8)


def last_kernel(rescale, coefs, sums, r_0, r_1, r_2, image_2, basis_out, hessenberg_out, basis, hessenberg, sems):
    moves = [pltpu.make_async_copy(basis.at[i], basis_out.at[i], sems.at[i]) for i in range(ITERS + 1)]
    moves.append(pltpu.make_async_copy(hessenberg, hessenberg_out, sems.at[ITERS + 1]))

    def put(i, value, scale):
        basis[i] = value * (lax.rsqrt(scale) * rescale)
        moves[i].start()

    taken_00, taken_01, taken_11, scale_0, scale_1, cross_01, norm_1 = [coefs[i : i + 1, :] for i in range(7)]
    put(0, r_0[...], scale_0)
    put(1, r_1[...], scale_1)
    total = sums[0]
    for k in range(1, sums.shape[0]):
        total = total + sums[k]
    queries = basis.shape[2]
    inner_0, inner_1, inner_2, norm_2, square = [total[:, i * queries : (i + 1) * queries] for i in range(5)]
    scale_2 = norm_2 + EPS * scale_1
    put(2, r_2[...], scale_2)
    norm_0 = scale_0 - EPS
    cross_02 = taken_01 * EPS - taken_11 * cross_01
    cross_12 = taken_11 * (EPS * scale_0)
    taken_0 = inner_0 / scale_0
    inner_1 = inner_1 - taken_0 * cross_01
    taken_1 = inner_1 / scale_1
    inner_2 = inner_2 - taken_0 * cross_02 - taken_1 * cross_12
    taken_2 = inner_2 / scale_2
    square = square - taken_0 * (2.0 * inner_0 - taken_0 * norm_0)
    square = square - taken_1 * (2.0 * inner_1 - taken_1 * norm_1)
    square = square - taken_2 * (2.0 * inner_2 - taken_2 * norm_2)
    scale_3 = jnp.maximum(square, 0.0) + EPS * scale_2
    put(3, image_2[...] - taken_0 * r_0[...] - taken_1 * r_1[...] - taken_2 * r_2[...], scale_3)
    scales = (scale_0, scale_1, scale_2, scale_3)
    inverse = [lax.rsqrt(scale) for scale in scales]
    root = [scale * inv for scale, inv in zip(scales, inverse)]
    hessenberg[...] = jnp.zeros(hessenberg.shape, F32)
    for step, column in enumerate(((taken_00,), (taken_01, taken_11), (taken_0, taken_1, taken_2))):
        for i, taken in enumerate(column):
            hessenberg[step, i : i + 1, :] = taken * root[i] * inverse[step]
        hessenberg[step, step + 1 : step + 2, :] = root[step + 1] * inverse[step]
    moves[ITERS + 1].start()
    for move in moves:
        move.wait()


def call(kernel, outs, *operands, scalars=0, scratch=(), aliases=None):
    vmem = pl.BlockSpec(memory_space=pltpu.VMEM)
    smem = pl.BlockSpec(memory_space=pltpu.SMEM)
    spaces = [pltpu.SMEM] * scalars + [pltpu.VMEM] * (len(operands) - scalars)
    operands = [pltpu.with_memory_space_constraint(x, space) for x, space in zip(operands, spaces)]
    return pl.pallas_call(
        kernel,
        out_shape=[pltpu.VMEM(shape, dtype) for shape, dtype in outs],
        in_specs=[smem] * scalars + [vmem] * (len(operands) - scalars),
        out_specs=[vmem] * len(outs),
        scratch_shapes=list(scratch),
        input_output_aliases=aliases or {},
        compiler_params=pltpu.CompilerParams(vmem_limit_bytes=VMEM_LIMIT),
    )(*operands)


def gather(message, shards, aside=None):
    blocks = [None] * shards
    blocks[0] = message
    for k in range(2, shards, 2):
        blocks[k] = lax.ppermute(message, "rows", partners(shards, k))
    if aside is not None:
        *blocks[2::2], aside = lax.optimization_barrier((*blocks[2::2], aside))
    for k in range(0, shards, 2):
        blocks[k + 1] = lax.ppermute(blocks[k], "rows", partners(shards, 1))
    return blocks, aside


def on_device(tiles, tile_row, tile_col, tile_count, damping, right_side):
    bands = lax.axis_size("band")
    shards = lax.axis_size("rows")
    slots = tiles.shape[2]
    width = right_side.shape[0]
    queries = right_side.shape[1]
    rescale = math.sqrt(width * bands * shards)
    damping = damping.reshape(1, queries)
    block = ((width, queries), F32)
    small = ((8, queries), F32)

    def message_shape(step):
        return (width + EXTRA[step], queries), BF16

    def multiply(step, blocks, *older):
        product = ((slots, width, queries), F32)
        (early,) = call(
            functools.partial(early_kernel, LATE),
            [product],
            plan,
            staged,
            *[block for k, block in enumerate(blocks) if k not in LATE],
            scalars=1,
            scratch=(pltpu.VMEM((width, queries), BF16),),
        )
        outs = [product, ((width + EXTRA[step], queries), F32)] + [message_shape(step)] * (bands - 1)
        if step == 1:
            outs.append(((slots + 8 - slots % 8, queries), F32))
        stored, *results = call(
            functools.partial(product_kernel, step, LATE, shards, bands, slots, width),
            outs,
            plan,
            staged,
            early,
            *blocks,
            *older,
            scalars=1,
            scratch=(pltpu.VMEM((shards, max(EXTRA[step], 8), queries), F32), pltpu.VMEM((bands, width, queries), F32)),
            aliases={2: 0},
        )
        parts = [results[0]] + [lax.ppermute(results[k], "band", partners(bands, k)) for k in reversed(range(1, bands))]
        return parts, [stored, *results[bands:]]

    smem = pl.BlockSpec(memory_space=pltpu.SMEM)
    vmem = pl.BlockSpec(memory_space=pltpu.VMEM)
    hbm = pl.BlockSpec(memory_space=pltpu.HBM)
    params = pltpu.CompilerParams(vmem_limit_bytes=VMEM_LIMIT)
    right_side, message = pl.pallas_call(
        open_kernel,
        out_shape=[pltpu.VMEM((width, queries), F32), pltpu.VMEM((width, queries), BF16)],
        in_specs=[hbm],
        out_specs=[vmem] * 2,
        scratch_shapes=[pltpu.SemaphoreType.DMA((4,))],
        compiler_params=params,
    )(pltpu.with_memory_space_constraint(right_side, pltpu.HBM))
    staged, plan = pl.pallas_call(
        stage_kernel,
        out_shape=[pltpu.VMEM(tiles.shape[2:], BF16), pltpu.SMEM((1, 1 + 2 * slots), jnp.int32)],
        in_specs=[hbm] * 3 + [smem, vmem],
        out_specs=[vmem, smem],
        scratch_shapes=[
            pltpu.SMEM(tile_row.shape, jnp.int32),
            pltpu.SMEM(tile_col.shape, jnp.int32),
            pltpu.SemaphoreType.DMA((3,)),
        ],
        compiler_params=params,
    )(
        *[pltpu.with_memory_space_constraint(x, pltpu.HBM) for x in (tiles, tile_row, tile_col)],
        tile_count,
        pltpu.with_memory_space_constraint(message, pltpu.VMEM),
    )
    blocks, (staged, plan) = gather(message, shards, (staged, plan))
    parts_0, (stored_0,) = multiply(0, blocks)
    image_0, message = call(functools.partial(first_kernel, bands), [block, message_shape(1)], damping, right_side, *parts_0)
    parts_1, (stored_1, side) = multiply(1, gather(message, shards)[0], stored_0)
    r_1, image_1, message, coefs = call(
        functools.partial(second_kernel, bands), [block, block, message_shape(2), small], damping, right_side, image_0, *parts_0, *parts_1
    )
    parts_2, _ = multiply(2, gather(message, shards)[0], stored_0, stored_1, side, coefs)
    r_2, image_2, sums, coefs = call(
        functools.partial(third_kernel, bands),
        [block, block, ((1, 5 * queries), F32), small],
        damping,
        right_side,
        r_1,
        image_1,
        coefs,
        *parts_0,
        *parts_1,
        *parts_2,
    )
    everyone = jnp.broadcast_to(sums[None], (bands * shards, *sums.shape))
    everyone = lax.all_to_all(everyone, ("rows", "band"), 0, 0, tiled=True)
    shapes = ((ITERS + 1, width, queries), (ITERS, ITERS + 1, queries))
    basis, hessenberg = pl.pallas_call(
        functools.partial(last_kernel, rescale),
        out_shape=[jax.ShapeDtypeStruct(shape, F32) for shape in shapes],
        in_specs=[vmem] * 6,
        out_specs=[pl.BlockSpec(memory_space=pltpu.HBM)] * 2,
        scratch_shapes=[pltpu.VMEM(shape, F32) for shape in shapes] + [pltpu.SemaphoreType.DMA((ITERS + 2,))],
        compiler_params=pltpu.CompilerParams(vmem_limit_bytes=VMEM_LIMIT),
    )(*[pltpu.with_memory_space_constraint(x, pltpu.VMEM) for x in (coefs, everyone, right_side, r_1, r_2, image_2)])
    return basis, jnp.swapaxes(hessenberg, 0, 1)


def solution(mesh):
    return jax.shard_map(
        lambda *args: tuple(on_device(*args)),
        mesh=mesh,
        in_specs=(
            P("rows", "band", None, None, None),
            P("rows", "band", None),
            P("rows", "band", None),
            P("rows", "band"),
            P(),
            P(("rows", "band"), None),
        ),
        out_specs=(P(None, ("rows", "band"), None), P()),
        check_vma=False,
    )
```

```python
import functools
import math

import jax
import jax.numpy as jnp
from jax import lax
from jax.experimental import pallas as pl
from jax.experimental.pallas import tpu as pltpu
from jax.sharding import PartitionSpec as P

ITERS = 3
EPS = 1e-06
EXTRA = (0, 8, 16)
VMEM_LIMIT = 16 << 20
LATE = (3, 5)
F32 = jnp.float32
BF16 = jnp.bfloat16


def partners(size, step):
    return [(i, i ^ step) for i in range(size)]


def pieces(value):
    high = value.astype(BF16).astype(F32)
    rest = value - high
    middle = rest.astype(BF16).astype(F32)
    return [high, middle, rest - middle]


def pack_rows(rows, count):
    place = lax.broadcasted_iota(jnp.int32, (count, rows[0].shape[1]), 0)
    packed = jnp.zeros(place.shape, F32)
    for index, row in enumerate(rows):
        packed = jnp.where(place == index, row, packed)
    return packed


def row_of(packed, index):
    return packed[index : index + 1, :]


def sum_of(packed, index):
    return row_of(packed, index) + row_of(packed, index + 1) + row_of(packed, index + 2)


def ratio(top, bottom):
    safe = jnp.where(bottom > 0, bottom, 1.0)
    return jnp.where(bottom > 0, top / safe, 0.0).astype(BF16).astype(F32)


def over_rows(value):
    return jnp.sum(value, axis=0, keepdims=True)


def open_kernel(right_side, r_0, message, sems):
    rows = right_side.shape[0] // sems.shape[0]
    spans = [pl.ds(i * rows, rows) for i in range(sems.shape[0])]
    moves = [pltpu.make_async_copy(right_side.at[span], r_0.at[span], sems.at[i]) for i, span in enumerate(spans)]
    for move in moves:
        move.start()
    for span, move in zip(spans, moves):
        move.wait()
        message[span, :] = r_0[span, :].astype(BF16)


def stage_kernel(tiles, row, col, count, after, staged, plan, rows, cols, sems):
    del after
    slots = row.shape[2]
    pairs = ((row, rows), (col, cols), (tiles.at[0, 0], staged))
    moves = [pltpu.make_async_copy(source, target, sems.at[i]) for i, (source, target) in enumerate(pairs)]
    for move in moves:
        move.start()
    for move in moves[:2]:
        move.wait()
    plan[0, 0] = count[0, 0]
    shard = lax.axis_index("rows")
    band = lax.axis_index("band")
    bands = lax.axis_size("band")
    for slot in range(slots):
        plan[0, 1 + slot] = cols[0, 0, slot] ^ shard
        plan[0, 1 + slots + slot] = (rows[0, 0, slot] - band + bands) % bands
    moves[2].wait()


def early_kernel(late, plan, tiles, *refs):
    *blocks, stored, column = refs
    slots, width, _ = stored.shape
    numbers = [k for k in range(len(blocks) + len(late)) if k not in late]
    for slot in range(slots):
        source = plan[0, 1 + slot]

        wait = functools.reduce(jnp.logical_or, [source == k for k in late])

        @pl.when((slot < plan[0, 0]) & jnp.logical_not(wait))
        def _(slot=slot, source=source):
            for k, block in zip(numbers, blocks):

                @pl.when(source == k)
                def _(block=block):
                    column[...] = block[:width, :]

            stored[slot] = jnp.dot(tiles[slot], column[...], preferred_element_type=F32)


def product_kernel(step, late, shards, bands, slots, width, *refs):
    refs = list(refs)
    take = lambda n: [refs.pop(0) for _ in range(n)]
    plan, tiles, early = take(3)
    blocks = take(shards)
    older = take(step)
    side, coefs = take(2) if step == 2 else (None, None)
    stored = take(1)[0]
    outs = take(bands)
    side_out = take(1)[0] if step == 1 else None
    extras, total = take(2)
    del early
    total[...] = jnp.zeros(total.shape, F32)
    rows = []
    wholes = []
    if step:
        for k in range(shards):
            extras[k] = blocks[k][width:, :].astype(F32)
        added = extras[0]
        for k in range(1, shards):
            added = added + extras[k]
        sums = [sum_of(added, step + 3 * i) for i in range(2 if step == 1 else 4)]
        if step == 1:
            wholes = [ratio(sums[0], sums[1])]
        else:
            inner_0, inner_1, norm_1, cross = sums
            whole_1 = ratio(inner_1, norm_1)
            wholes = [ratio(inner_0 - whole_1 * cross, side[slots : slots + 1, :]), whole_1]
        rows = wholes + [piece for value in sums for piece in pieces(value)]
    if side_out is not None:
        side_out[...] = jnp.zeros(side_out.shape, F32)
        side_out[slots : slots + 1, :] = sums[1]
    for slot in range(slots):

        @pl.when(slot < plan[0, 0])
        def _(slot=slot):
            source = plan[0, 1 + slot]
            target = plan[0, 1 + slots + slot]

            for k in late:

                @pl.when(source == k)
                def _(k=k):
                    stored[slot] = jnp.dot(tiles[slot], blocks[k][:width, :], preferred_element_type=F32)

            product = stored[slot]
            if step:
                extra = extras[source]
                if step == 1:
                    own = row_of(extra, 0)
                    side_out[slot : slot + 1, :] = own
                    product = product + (own - wholes[0]) * older[0][slot]
                else:
                    first = row_of(extra, 0) - wholes[0]
                    second = row_of(extra, 1) - wholes[1]
                    first = first + second * (side[slot : slot + 1, :] - coefs[0:1, :])
                    product = product + second * older[1][slot] + first * older[0][slot]
            total[target] += product

    outs[0][:width, :] = total[0]
    for k in range(1, bands):
        outs[k][:width, :] = total[k].astype(BF16)
    if step:
        packed = pack_rows(rows, EXTRA[step])
        outs[0][width:, :] = packed
        for k in range(1, bands):
            outs[k][width:, :] = packed.astype(BF16)


def message_of(message, value, coefs, sums):
    width = value.shape[0]
    message[:width, :] = value.astype(BF16)
    rows = coefs + [piece for entry in sums for piece in pieces(entry)]
    message[width:, :] = pack_rows(rows, message.shape[0] - width).astype(BF16)


def first_kernel(bands, damping, r_0, *refs):
    parts = refs[:bands]
    image_out, message = refs[bands:]
    r = r_0[...]
    image = damping[...] * r
    for part in parts:
        image = image + part[...].astype(F32)
    image_out[...] = image
    inner = over_rows(r * image)
    norm = over_rows(r * r)
    own = ratio(inner, norm)
    message_of(message, image - own * r, [own], [inner, norm])


def global_sums(parts, width, step, count):
    packed = parts[0][width:, :].astype(F32)
    for part in parts[1:]:
        packed = packed + part[width:, :].astype(F32)
    return [sum_of(packed, step + 3 * i) for i in range(count)]


def second_kernel(bands, damping, r_0, image_0, *refs):
    first = refs[:bands]
    parts = refs[bands : 2 * bands]
    r_1_out, image_out, message, coefs = refs[2 * bands :]
    width = r_0.shape[0]
    inner, norm = global_sums(parts, width, 1, 2)
    scale_0 = norm + EPS
    taken = inner / scale_0
    r0 = r_0[...]
    r1 = image_0[...] - taken * r0
    r_1_out[...] = r1
    image = damping[...] * r1
    for old, part in zip(first, parts):
        back = part[width : width + 1, :].astype(F32) - taken
        image = image + part[:width, :].astype(F32) + back * old[...].astype(F32)
    image_out[...] = image
    inner_0 = over_rows(r0 * image)
    inner_1 = over_rows(r1 * image)
    norm_1 = over_rows(r1 * r1)
    cross = over_rows(r0 * r1)
    own_1 = ratio(inner_1, norm_1)
    rest = image - own_1 * r1
    own_0 = ratio(over_rows(r0 * rest), over_rows(r0 * r0))
    message_of(message, rest - own_0 * r0, [own_0, own_1], [inner_0, inner_1, norm_1, cross])
    coefs[...] = pack_rows([taken, scale_0], 8)


def third_kernel(bands, damping, r_0, r_1, image_1, coefs, *refs):
    first = refs[:bands]
    second = refs[bands : 2 * bands]
    parts = refs[2 * bands : 3 * bands]
    r_2_out, image_out, sums_out, coefs_out = refs[3 * bands :]
    width = r_0.shape[0]
    inner_0, inner_1, norm_1, cross = global_sums(parts, width, 2, 4)
    taken_00 = coefs[0:1, :]
    scale_0 = coefs[1:2, :]
    scale_1 = norm_1 + EPS * scale_0
    taken_0 = inner_0 / scale_0
    taken_1 = (inner_1 - taken_0 * cross) / scale_1
    r0 = r_0[...]
    r1 = r_1[...]
    r2 = image_1[...] - taken_0 * r0 - taken_1 * r1
    r_2_out[...] = r2
    image = damping[...] * r2
    for old_0, old_1, part in zip(first, second, parts):
        back_0 = part[width : width + 1, :].astype(F32) - taken_0
        back_1 = part[width + 1 : width + 2, :].astype(F32) - taken_1
        back_0 = back_0 + back_1 * (old_1[width : width + 1, :].astype(F32) - taken_00)
        image = image + part[:width, :].astype(F32)
        image = image + back_1 * old_1[:width, :].astype(F32) + back_0 * old_0[...].astype(F32)
    image_out[...] = image
    queries = r0.shape[1]
    for i, (a, b) in enumerate(((r0, image), (r1, image), (r2, image), (r2, r2), (image, image))):
        sums_out[:, i * queries : (i + 1) * queries] = over_rows(a * b)
    coefs_out[...] = pack_rows([taken_00, taken_0, taken_1, scale_0, scale_1, cross, norm_1], 8)


def last_kernel(rescale, coefs, sums, r_0, r_1, r_2, image_2, basis_out, hessenberg_out, basis, hessenberg, sems):
    moves = [pltpu.make_async_copy(basis.at[i], basis_out.at[i], sems.at[i]) for i in range(ITERS + 1)]
    moves.append(pltpu.make_async_copy(hessenberg, hessenberg_out, sems.at[ITERS + 1]))

    def put(i, value, scale):
        basis[i] = value * (lax.rsqrt(scale) * rescale)
        moves[i].start()

    taken_00, taken_01, taken_11, scale_0, scale_1, cross_01, norm_1 = [coefs[i : i + 1, :] for i in range(7)]
    put(0, r_0[...], scale_0)
    put(1, r_1[...], scale_1)
    total = sums[0]
    for k in range(1, sums.shape[0]):
        total = total + sums[k]
    queries = basis.shape[2]
    inner_0, inner_1, inner_2, norm_2, square = [total[:, i * queries : (i + 1) * queries] for i in range(5)]
    scale_2 = norm_2 + EPS * scale_1
    put(2, r_2[...], scale_2)
    norm_0 = scale_0 - EPS
    cross_02 = taken_01 * EPS - taken_11 * cross_01
    cross_12 = taken_11 * (EPS * scale_0)
    taken_0 = inner_0 / scale_0
    inner_1 = inner_1 - taken_0 * cross_01
    taken_1 = inner_1 / scale_1
    inner_2 = inner_2 - taken_0 * cross_02 - taken_1 * cross_12
    taken_2 = inner_2 / scale_2
    square = square - taken_0 * (2.0 * inner_0 - taken_0 * norm_0)
    square = square - taken_1 * (2.0 * inner_1 - taken_1 * norm_1)
    square = square - taken_2 * (2.0 * inner_2 - taken_2 * norm_2)
    scale_3 = jnp.maximum(square, 0.0) + EPS * scale_2
    put(3, image_2[...] - taken_0 * r_0[...] - taken_1 * r_1[...] - taken_2 * r_2[...], scale_3)
    scales = (scale_0, scale_1, scale_2, scale_3)
    inverse = [lax.rsqrt(scale) for scale in scales]
    root = [scale * inv for scale, inv in zip(scales, inverse)]
    hessenberg[...] = jnp.zeros(hessenberg.shape, F32)
    for step, column in enumerate(((taken_00,), (taken_01, taken_11), (taken_0, taken_1, taken_2))):
        for i, taken in enumerate(column):
            hessenberg[step, i : i + 1, :] = taken * root[i] * inverse[step]
        hessenberg[step, step + 1 : step + 2, :] = root[step + 1] * inverse[step]
    moves[ITERS + 1].start()
    for move in moves:
        move.wait()


def call(kernel, outs, *operands, scalars=0, scratch=(), aliases=None):
    vmem = pl.BlockSpec(memory_space=pltpu.VMEM)
    smem = pl.BlockSpec(memory_space=pltpu.SMEM)
    spaces = [pltpu.SMEM] * scalars + [pltpu.VMEM] * (len(operands) - scalars)
    operands = [pltpu.with_memory_space_constraint(x, space) for x, space in zip(operands, spaces)]
    return pl.pallas_call(
        kernel,
        out_shape=[pltpu.VMEM(shape, dtype) for shape, dtype in outs],
        in_specs=[smem] * scalars + [vmem] * (len(operands) - scalars),
        out_specs=[vmem] * len(outs),
        scratch_shapes=list(scratch),
        input_output_aliases=aliases or {},
        compiler_params=pltpu.CompilerParams(vmem_limit_bytes=VMEM_LIMIT),
    )(*operands)


def gather(message, shards, aside=None):
    blocks = [None] * shards
    blocks[0] = message
    for k in range(2, shards, 2):
        blocks[k] = lax.ppermute(message, "rows", partners(shards, k))
    if aside is not None:
        *blocks[2::2], aside = lax.optimization_barrier((*blocks[2::2], aside))
    for k in range(0, shards, 2):
        blocks[k + 1] = lax.ppermute(blocks[k], "rows", partners(shards, 1))
    return blocks, aside


def on_device(tiles, tile_row, tile_col, tile_count, damping, right_side):
    bands = lax.axis_size("band")
    shards = lax.axis_size("rows")
    slots = tiles.shape[2]
    width = right_side.shape[0]
    queries = right_side.shape[1]
    rescale = math.sqrt(width * bands * shards)
    damping = damping.reshape(1, queries)
    block = ((width, queries), F32)
    small = ((8, queries), F32)

    def message_shape(step):
        return (width + EXTRA[step], queries), BF16

    def multiply(step, blocks, *older):
        product = ((slots, width, queries), F32)
        (early,) = call(
            functools.partial(early_kernel, LATE),
            [product],
            plan,
            staged,
            *[block for k, block in enumerate(blocks) if k not in LATE],
            scalars=1,
            scratch=(pltpu.VMEM((width, queries), BF16),),
        )
        outs = [product, ((width + EXTRA[step], queries), F32)] + [message_shape(step)] * (bands - 1)
        if step == 1:
            outs.append(((slots + 8 - slots % 8, queries), F32))
        stored, *results = call(
            functools.partial(product_kernel, step, LATE, shards, bands, slots, width),
            outs,
            plan,
            staged,
            early,
            *blocks,
            *older,
            scalars=1,
            scratch=(pltpu.VMEM((shards, max(EXTRA[step], 8), queries), F32), pltpu.VMEM((bands, width, queries), F32)),
            aliases={2: 0},
        )
        shifts = sorted(range(1, bands), key=lambda k: (k != bands // 2, k))
        parts = [results[0]]
        for k in shifts:
            parts.append(lax.ppermute(results[k], "band", [(i, (i + k) % bands) for i in range(bands)]))
        return parts, [stored, *results[bands:]]

    smem = pl.BlockSpec(memory_space=pltpu.SMEM)
    vmem = pl.BlockSpec(memory_space=pltpu.VMEM)
    hbm = pl.BlockSpec(memory_space=pltpu.HBM)
    params = pltpu.CompilerParams(vmem_limit_bytes=VMEM_LIMIT)
    right_side, message = pl.pallas_call(
        open_kernel,
        out_shape=[pltpu.VMEM((width, queries), F32), pltpu.VMEM((width, queries), BF16)],
        in_specs=[hbm],
        out_specs=[vmem] * 2,
        scratch_shapes=[pltpu.SemaphoreType.DMA((4,))],
        compiler_params=params,
    )(pltpu.with_memory_space_constraint(right_side, pltpu.HBM))
    staged, plan = pl.pallas_call(
        stage_kernel,
        out_shape=[pltpu.VMEM(tiles.shape[2:], BF16), pltpu.SMEM((1, 1 + 2 * slots), jnp.int32)],
        in_specs=[hbm] * 3 + [smem, vmem],
        out_specs=[vmem, smem],
        scratch_shapes=[
            pltpu.SMEM(tile_row.shape, jnp.int32),
            pltpu.SMEM(tile_col.shape, jnp.int32),
            pltpu.SemaphoreType.DMA((3,)),
        ],
        compiler_params=params,
    )(
        *[pltpu.with_memory_space_constraint(x, pltpu.HBM) for x in (tiles, tile_row, tile_col)],
        tile_count,
        pltpu.with_memory_space_constraint(message, pltpu.VMEM),
    )
    blocks, (staged, plan) = gather(message, shards, (staged, plan))
    parts_0, (stored_0,) = multiply(0, blocks)
    image_0, message = call(functools.partial(first_kernel, bands), [block, message_shape(1)], damping, right_side, *parts_0)
    parts_1, (stored_1, side) = multiply(1, gather(message, shards)[0], stored_0)
    r_1, image_1, message, coefs = call(
        functools.partial(second_kernel, bands), [block, block, message_shape(2), small], damping, right_side, image_0, *parts_0, *parts_1
    )
    parts_2, _ = multiply(2, gather(message, shards)[0], stored_0, stored_1, side, coefs)
    r_2, image_2, sums, coefs = call(
        functools.partial(third_kernel, bands),
        [block, block, ((1, 5 * queries), F32), small],
        damping,
        right_side,
        r_1,
        image_1,
        coefs,
        *parts_0,
        *parts_1,
        *parts_2,
    )
    everyone = jnp.broadcast_to(sums[None], (bands * shards, *sums.shape))
    everyone = lax.all_to_all(everyone, ("rows", "band"), 0, 0, tiled=True)
    shapes = ((ITERS + 1, width, queries), (ITERS, ITERS + 1, queries))
    basis, hessenberg = pl.pallas_call(
        functools.partial(last_kernel, rescale),
        out_shape=[jax.ShapeDtypeStruct(shape, F32) for shape in shapes],
        in_specs=[vmem] * 6,
        out_specs=[pl.BlockSpec(memory_space=pltpu.HBM)] * 2,
        scratch_shapes=[pltpu.VMEM(shape, F32) for shape in shapes] + [pltpu.SemaphoreType.DMA((ITERS + 2,))],
        compiler_params=pltpu.CompilerParams(vmem_limit_bytes=VMEM_LIMIT),
    )(*[pltpu.with_memory_space_constraint(x, pltpu.VMEM) for x in (coefs, everyone, right_side, r_1, r_2, image_2)])
    return basis, jnp.swapaxes(hessenberg, 0, 1)


def solution(mesh):
    return jax.shard_map(
        lambda *args: tuple(on_device(*args)),
        mesh=mesh,
        in_specs=(
            P("rows", "band", None, None, None),
            P("rows", "band", None),
            P("rows", "band", None),
            P("rows", "band"),
            P(),
            P(("rows", "band"), None),
        ),
        out_specs=(P(None, ("rows", "band"), None), P()),
        check_vma=False,
    )
```
